8 devices in a mesh: dp: 1 (over z), dm: 2 (over y), tp: 4 (over x, core).
Axes of the slice: x: 2, y: 2, z: 1, core: 2. Of those that a mesh axis runs over, the one named last changes fastest.
Arguments:
- hidden: bfloat16 [128, 8192], P('dp', 'dm')
- w_q: bfloat16 [8192, 64, 128], P('dm', 'tp')
- w_k: bfloat16 [8192, 8, 128], P('dm', 'tp')
- w_v: bfloat16 [8192, 8, 128], P('dm', 'tp')
- w_o: bfloat16 [64, 128, 8192], P('tp', None, 'dm')
- w_gate: bfloat16 [8192, 22016], P('dm', 'tp')
- w_up: bfloat16 [8192, 22016], P('dm', 'tp')
- w_down: bfloat16 [22016, 8192], P('tp', 'dm')
- norm_attn: bfloat16 [8192], P('dm')
- norm_mlp: bfloat16 [8192], P('dm')
- k_cache: bfloat16 [128, 128, 8, 128], P(('dp', 'dm'), None, 'tp')
- v_cache: bfloat16 [128, 128, 8, 128], P(('dp', 'dm'), None, 'tp')
- seq_lens: int32 [128], P(('dp', 'dm'))
- rope_cos: float32 [128, 64], P(('dp', 'dm'))
- rope_sin: float32 [128, 64], P(('dp', 'dm'))
Outputs:
- output 1: bfloat16 [128, 8192], P('dp', 'dm')
- output 2: bfloat16 [128, 128, 8, 128], P(('dp', 'dm'), None, 'tp')
- output 3: bfloat16 [128, 128, 8, 128], P(('dp', 'dm'), None, 'tp')
All inputs are finite; a program needn't handle non-finite values.
Results may differ from the reference program's by a relative error of at most 0.0105769.
Values are sent between devices in bfloat16 or wider.
A program may use at most 1 GiB of HBM per device.

```python
import math
import jax
import jax.numpy as jnp
from jax import lax

D = 8192
HEADS = 64
KV_HEADS = 8
HEAD = 128
FF = 22016
BATCH = 128
SEQ = 128

GROUP = HEADS // KV_HEADS
HALF = HEAD // 2
EPS = 1e-6
ROPE_BASE = 10000.0
K_SCALE = math.sqrt(max(math.log(SEQ / 16.0), 1.0))


def rope_tables(seq_lens):
    inv_freq = ROPE_BASE ** (-2.0 * jnp.arange(HALF, dtype=jnp.float32) / HEAD)
    angles = seq_lens.astype(jnp.float32)[:, None] * inv_freq[None, :]
    return jnp.cos(angles), jnp.sin(angles)


def draw_lengths(key):
    lengths = jax.random.randint(key, (BATCH,), SEQ // 8, SEQ, dtype=jnp.int32)
    return lengths.at[0].set(SEQ - 1).at[BATCH - 1].set(SEQ // 8)


def setup_inputs(seed: int = 0, part: int = 0) -> dict:
    shared = jax.random.split(jax.random.key(seed), 9)
    local = jax.random.split(jax.random.fold_in(jax.random.key(seed), part), 4)
    w_q = (jax.random.normal(shared[0], (D, HEADS, HEAD), jnp.float32) * D ** -0.5).astype(jnp.bfloat16)
    w_k = (jax.random.normal(shared[1], (D, KV_HEADS, HEAD), jnp.float32) * (K_SCALE * D ** -0.5)).astype(jnp.bfloat16)
    w_v = (jax.random.normal(shared[2], (D, KV_HEADS, HEAD), jnp.float32) * D ** -0.5).astype(jnp.bfloat16)
    w_o = (jax.random.normal(shared[3], (HEADS, HEAD, D), jnp.float32) * (HEADS * HEAD) ** -0.5).astype(jnp.bfloat16)
    w_gate = (jax.random.normal(shared[4], (D, FF), jnp.float32) * D ** -0.5).astype(jnp.bfloat16)
    w_up = (jax.random.normal(shared[5], (D, FF), jnp.float32) * D ** -0.5).astype(jnp.bfloat16)
    w_down = (jax.random.normal(shared[6], (FF, D), jnp.float32) * FF ** -0.5).astype(jnp.bfloat16)
    norm_attn = (1.0 + 0.4 * jax.random.normal(shared[7], (D,), jnp.float32)).astype(jnp.bfloat16)
    norm_mlp = (1.0 + 0.4 * jax.random.normal(shared[8], (D,), jnp.float32)).astype(jnp.bfloat16)
    hidden = jax.random.normal(local[0], (BATCH, D), jnp.float32).astype(jnp.bfloat16)
    k_cache = (jax.random.normal(local[1], (BATCH, SEQ, KV_HEADS, HEAD), jnp.float32) * K_SCALE).astype(jnp.bfloat16)
    v_cache = jax.random.normal(local[2], (BATCH, SEQ, KV_HEADS, HEAD), jnp.float32).astype(jnp.bfloat16)
    seq_lens = draw_lengths(local[3])
    rope_cos, rope_sin = rope_tables(seq_lens)
    return dict(hidden=hidden, w_q=w_q, w_k=w_k, w_v=w_v, w_o=w_o, w_gate=w_gate, w_up=w_up, w_down=w_down, norm_attn=norm_attn, norm_mlp=norm_mlp, k_cache=k_cache, v_cache=v_cache, seq_lens=seq_lens, rope_cos=rope_cos, rope_sin=rope_sin)


def rms_norm(x, gain):
    x_f32 = x.astype(jnp.float32)
    scale = lax.rsqrt(jnp.mean(x_f32 * x_f32, axis=-1, keepdims=True) + EPS)
    return (x_f32 * scale * gain.astype(jnp.float32)).astype(jnp.bfloat16)


def apply_rope(x, rope_cos, rope_sin):
    first = x[..., :HALF]
    second = x[..., HALF:]
    cosine = rope_cos[:, None, :]
    sine = rope_sin[:, None, :]
    return jnp.concatenate([first * cosine - second * sine, second * cosine + first * sine], axis=-1).astype(jnp.bfloat16)


def project(x, weight):
    return jnp.dot(x, weight.reshape(D, -1), preferred_element_type=jnp.float32).reshape(BATCH, -1, HEAD)


def attend_row(row_args):
    q_row, k_row, v_row, length = row_args
    q_grp = q_row.reshape(KV_HEADS, GROUP, HEAD).astype(jnp.float32)
    scores = jnp.einsum('kgd,skd->kgs', q_grp, k_row.astype(jnp.float32)) / math.sqrt(HEAD)
    key_mask = jnp.arange(SEQ)[None, None, :] <= length
    scores = jnp.where(key_mask, scores, -1e30)
    attn_probs = jax.nn.softmax(scores, axis=-1).astype(jnp.bfloat16).astype(jnp.float32)
    heads = jnp.einsum('kgs,skd->kgd', attn_probs, v_row.astype(jnp.float32))
    return heads.reshape(HEADS, HEAD).astype(jnp.bfloat16)


def reference(hidden, w_q, w_k, w_v, w_o, w_gate, w_up, w_down, norm_attn, norm_mlp, k_cache, v_cache, seq_lens, rope_cos, rope_sin):
    x_norm = rms_norm(hidden, norm_attn)
    q_rot = apply_rope(project(x_norm, w_q), rope_cos, rope_sin)
    k_rot = apply_rope(project(x_norm, w_k), rope_cos, rope_sin)
    v_new = project(x_norm, w_v).astype(jnp.bfloat16)
    write_mask = (jnp.arange(SEQ)[None, :] == seq_lens[:, None])[:, :, None, None]
    k_out = jnp.where(write_mask, k_rot[:, None], k_cache)
    v_out = jnp.where(write_mask, v_new[:, None], v_cache)
    attn_heads = lax.map(attend_row, (q_rot, k_out, v_out, seq_lens))
    attn_out = jnp.dot(attn_heads.reshape(BATCH, HEADS * HEAD), w_o.reshape(HEADS * HEAD, D), preferred_element_type=jnp.float32).astype(jnp.bfloat16)
    h_mid = hidden + attn_out
    x_mlp = rms_norm(h_mid, norm_mlp)
    gate = jnp.dot(x_mlp, w_gate, preferred_element_type=jnp.float32)
    up_proj = jnp.dot(x_mlp, w_up, preferred_element_type=jnp.float32)
    gated_act = (jax.nn.silu(gate) * up_proj).astype(jnp.bfloat16)
    mlp_out = jnp.dot(gated_act, w_down, preferred_element_type=jnp.float32).astype(jnp.bfloat16)
    return (h_mid + mlp_out, k_out, v_out)
```

```python
import functools

import jax
import jax.numpy as jnp
from jax import lax
from jax.experimental import pallas as pl
from jax.experimental.pallas import tpu as pltpu
from jax.sharding import PartitionSpec as P

EPS = 1e-6
MESH = pl.DeviceIdType.MESH
F32 = jnp.float32
BF16 = jnp.bfloat16
ANY = pl.BlockSpec(memory_space=pl.ANY)
VM = pl.BlockSpec(memory_space=pltpu.VMEM)
SM = pl.BlockSpec(memory_space=pltpu.SMEM)


def me():
    return lax.axis_index('dp'), lax.axis_index('dm'), lax.axis_index('tp')


def row_to_lanes(col):
    return jnp.broadcast_to(col, (128, 128)).T[0:8, :]


def lanes_to_row(vec):
    return jnp.broadcast_to(vec, (128, 128)).T[:, 0:1]


def norm_kernel(width_full, h_ref, g_ref, x_ref, mine, theirs, ssem, rsem):
    dp, dm, tp = me()
    peer = (dp, 1 - dm, tp)
    bar = pltpu.get_barrier_semaphore()
    pl.semaphore_signal(bar, inc=1, device_id=peer, device_id_type=MESH)
    h = h_ref[...].astype(F32)
    mine[...] = row_to_lanes(jnp.sum(h * h, axis=-1, keepdims=True))
    pl.semaphore_wait(bar, 1)
    cp = pltpu.make_async_remote_copy(mine, theirs, ssem, rsem, device_id=peer, device_id_type=MESH)
    cp.start()
    cp.wait()
    total = lanes_to_row(mine[0:1, :] + theirs[0:1, :])
    scale = lax.rsqrt(total / width_full + EPS)
    for r in range(4):
        rows = slice(32 * r, 32 * r + 32)
        x_ref[rows, :] = (h_ref[rows, :].astype(F32) * scale[rows, :] * g_ref[...].astype(F32)).astype(BF16)


def norm_call(hidden, gain, width_full):
    return pl.pallas_call(
        functools.partial(norm_kernel, width_full),
        out_shape=jax.ShapeDtypeStruct(hidden.shape, BF16),
        in_specs=[VM, VM], out_specs=VM,
        scratch_shapes=[pltpu.VMEM((8, 128), F32), pltpu.VMEM((8, 128), F32), pltpu.SemaphoreType.DMA, pltpu.SemaphoreType.DMA],
        compiler_params=pltpu.CompilerParams(collective_id=0, has_side_effects=True, vmem_limit_bytes=24 * 2**20),
        name='norm_x',
    )(hidden, gain)


QCH = 8


def rope_kernel(q_ref, kv_ref, cos_ref, sin_ref, qo_ref, kvo_ref, qbuf, kvbuf, ss, rs):
    dp, dm, tp = me()
    peer = (dp, 1 - dm, tp)
    mine = pl.ds(pl.multiple_of(dm * 64, 64), 64)
    other = pl.ds(pl.multiple_of((1 - dm) * 64, 64), 64)
    bar = pltpu.get_barrier_semaphore()
    pl.semaphore_signal(bar, inc=1, device_id=peer, device_id_type=MESH)
    pl.semaphore_wait(bar, 1)
    cps = []
    for i in range(QCH):
        n = 16 // QCH
        cps.append(pltpu.make_async_remote_copy(q_ref.at[i * n:(i + 1) * n, other, :], qbuf.at[i * n:(i + 1) * n], ss.at[i], rs.at[i],
                                                device_id=peer, device_id_type=MESH))
    cps.append(pltpu.make_async_remote_copy(kv_ref.at[:, other, :], kvbuf, ss.at[QCH], rs.at[QCH], device_id=peer, device_id_type=MESH))
    for cp in cps:
        cp.start()
    c = cos_ref[...]
    s = sin_ref[...]
    cos2 = jnp.concatenate([c, c], axis=-1)
    sin2 = jnp.concatenate([-s, s], axis=-1)

    def rope(a):
        return (a * cos2 + pltpu.roll(a, 64, 1) * sin2).astype(BF16)

    for i in range(QCH):
        cps[i].wait_recv()
        for h in range(i * (16 // QCH), (i + 1) * (16 // QCH)):
            qo_ref[h] = rope(q_ref[h, mine, :] + qbuf[h])
    cps[QCH].wait_recv()
    for h in range(2):
        kvo_ref[h] = rope(kv_ref[h, mine, :] + kvbuf[h])
        kvo_ref[2 + h] = (kv_ref[2 + h, mine, :] + kvbuf[2 + h]).astype(BF16)
    for cp in cps:
        cp.wait_send()


def rope_call(q_part, kv_part, cos, sin):
    return pl.pallas_call(
        rope_kernel,
        out_shape=(jax.ShapeDtypeStruct((16, 64, 128), BF16), jax.ShapeDtypeStruct((4, 64, 128), BF16)),
        in_specs=[VM] * 4, out_specs=(VM, VM),
        scratch_shapes=[pltpu.VMEM((16, 64, 128), F32), pltpu.VMEM((4, 64, 128), F32), pltpu.SemaphoreType.DMA((QCH + 1,)), pltpu.SemaphoreType.DMA((QCH + 1,))],
        compiler_params=pltpu.CompilerParams(collective_id=1, has_side_effects=True, vmem_limit_bytes=24 * 2**20),
        name='rs_rope',
    )(q_part, kv_part, cos, sin)


ACH = 4
AROWS = 64 // ACH


def attn_kernel(q_ref, kv_ref, len_ref, kc, vc, ko, vo, o_ref, kb, vb, qs, os, isem, osem):
    def cin(ch, t):
        rows = pl.ds(ch * AROWS, AROWS)
        return pltpu.make_async_copy((kc, vc)[t].at[rows], (kb, vb)[t].at[rows], isem.at[t, ch])

    def cout(ch, t):
        rows = pl.ds(ch * AROWS, AROWS)
        return pltpu.make_async_copy((kb, vb)[t].at[rows], (ko, vo)[t].at[rows], osem.at[t, ch])

    for ch in range(ACH):
        for t in range(2):
            cin(ch, t).start()
    for h in range(16):
        qs[pl.ds(h, 64, stride=16), :] = q_ref[h].astype(F32)
    row16 = lax.broadcasted_iota(jnp.int32, (16, 128), 0)
    col = lax.broadcasted_iota(jnp.int32, (16, 256), 1)
    head = lax.broadcasted_iota(jnp.int32, (16, 256), 0)
    own = lax.rem(col, 2) == head // 8

    @pl.loop(0, ACH)
    def _(ch):
        cin(ch, 0).wait()
        cin(ch, 1).wait()
        kv32 = [kv_ref[j, pl.ds(pl.multiple_of(ch * AROWS, AROWS), AROWS), :].astype(F32) for j in range(4)]
        for i in range(AROWS):
            b = ch * AROWS + i
            ln = len_ref[b]
            t8 = ln // 8
            at = pl.ds(pl.multiple_of(t8 * 16, 16), 16)
            r0 = 2 * (ln - 8 * t8)
            for t, buf in enumerate((kb, vb)):
                old = buf[b, at, :].astype(F32)
                n0 = jnp.broadcast_to(kv32[2 * t][i:i + 1, :], (16, 128))
                n1 = jnp.broadcast_to(kv32[2 * t + 1][i:i + 1, :], (16, 128))
                new = jnp.where(row16 == r0, n0, jnp.where(row16 == r0 + 1, n1, old))
                buf[b, at, :] = new.astype(BF16)
        cout(ch, 0).start()
        cout(ch, 1).start()
        for i in range(AROWS):
            b = ch * AROWS + i
            ln = len_ref[b]
            q = qs[pl.ds(pl.multiple_of(b * 16, 16), 16), :].astype(BF16)
            s = lax.dot_general(q, kb[b], (((1,), (1,)), ((), ())), preferred_element_type=F32) * (128.0 ** -0.5)
            s = jnp.where(own & (col <= 2 * ln + 1), s, -1e30)
            p = jnp.exp(s - jnp.max(s, axis=-1, keepdims=True))
            p = (p / jnp.sum(p, axis=-1, keepdims=True)).astype(BF16)
            os[pl.ds(pl.multiple_of(b * 16, 16), 16), :] = jnp.dot(p, vb[b], preferred_element_type=F32)

    for h in range(16):
        o_ref[:, h * 128:(h + 1) * 128] = os[pl.ds(h, 64, stride=16), :].astype(BF16)
    for ch in range(ACH):
        cout(ch, 0).wait()
        cout(ch, 1).wait()


def attn_call(q_rot, kv_new, seq_lens, k_cache, v_cache):
    cache = jax.ShapeDtypeStruct((64, 256, 128), BF16)
    return pl.pallas_call(
        attn_kernel,
        out_shape=(cache, cache, jax.ShapeDtypeStruct((64, 2048), BF16)),
        in_specs=[VM, VM, SM, ANY, ANY], out_specs=(ANY, ANY, VM),
        scratch_shapes=[pltpu.VMEM((64, 256, 128), BF16), pltpu.VMEM((64, 256, 128), BF16), pltpu.VMEM((1024, 128), F32), pltpu.VMEM((1024, 128), F32),
                        pltpu.SemaphoreType.DMA((2, ACH)), pltpu.SemaphoreType.DMA((2, ACH))],
        compiler_params=pltpu.CompilerParams(vmem_limit_bytes=32 * 2**20),
        name='attend',
    )(q_rot, kv_new, seq_lens, k_cache, v_cache)


C = 256
N = 22
NB = 3
ND = 8
NR = 4
RB = 128 // NR
LAG = 2
DLAG = 4


def mlp_kernel(width_full, o_ref, hid, gain, wo, wg, wu, wd, out,
               wbuf, dbuf, oall, acc, dd, xs, xr, hq, oq, x2, gown, gsnd, grcv, mall, st,
               wsem, dsem, osem, d2d, xx, agc, agx, fwd, stsem, gs, gr, ms, mr):
    dp, dm, tp = me()
    x = tp // 2
    c = lax.rem(tp, 2)
    ypeer = (dp, 1 - dm, tp)
    cpeer = (dp, dm, x * 2 + 1 - c)
    xpeer = (dp, dm, (1 - x) * 2 + c)
    flat = dm * 4 + tp

    def at_flat(k):
        f = lax.rem(flat + k, 8)
        return f, (dp, f // 4, lax.rem(f, 4))

    def rdma(src, dst, s, r, dev):
        return pltpu.make_async_remote_copy(src, dst, s, r, device_id=dev, device_id_type=MESH)

    def half(d):
        return pl.ds(pl.multiple_of(d * 64, 64), 64)

    def col(ch):
        return pl.multiple_of(ch * C - 128, 128)

    def wcopy(ch, t):
        slot = lax.rem(ch, NB)
        return pltpu.make_async_copy((wg, wu)[t].at[:, pl.ds(col(ch), C)], wbuf.at[slot, t], wsem.at[slot, t])

    def wcopy0(t):
        return pltpu.make_async_copy((wg, wu)[t].at[:, 0:128], wbuf.at[0, t, :, 0:128], wsem.at[0, t])

    def ocopy(j):
        return pltpu.make_async_copy(wo.at[j * C:(j + 1) * C], dbuf.at[j], dsem.at[j])

    def dslot(ch):
        return lax.rem(ch, ND)

    def dcopy(ch):
        slot = dslot(ch)
        return pltpu.make_async_copy(wd.at[pl.ds(col(ch), C)], dbuf.at[slot], dsem.at[slot])

    def dcopy0():
        return pltpu.make_async_copy(wd.at[0:128], dbuf.at[0, 0:128], dsem.at[0])

    for j in range(8):
        ocopy(j).start()

    bar = pltpu.get_barrier_semaphore()
    for k in range(1, 8):
        pl.semaphore_signal(bar, inc=1, device_id=at_flat(k)[1], device_id_type=MESH)
    for t in range(2):
        wcopy0(t).start()
    for ch in range(1, NB):
        for t in range(2):
            wcopy(ch, t).start()
    pl.semaphore_wait(bar, 7)
    ocp = rdma(o_ref, oall, osem.at[0], osem.at[1], ypeer)
    ocp.start()

    def blk(r):
        return slice(r * RB, (r + 1) * RB)

    def d2d_cp(u, r):
        return rdma(acc.at[1 - c, :, blk(r), :], dd.at[:, blk(r), :], d2d.at[u, 0, r], d2d.at[u, 1, r], cpeer)

    def x_cp(u, r):
        return rdma(xs.at[blk(r)], xr.at[blk(r)], xx.at[u, 0, r], xx.at[u, 1, r], xpeer)

    def agc_cp(u, r, buf):
        return rdma(buf.at[tp, blk(r)], buf.at[tp, blk(r)], agc.at[u, 0, r], agc.at[u, 1, r], cpeer)

    def agx_cp(u, r, buf):
        return rdma(buf.at[tp, blk(r)], buf.at[tp, blk(r)], agx.at[u, 0, r], agx.at[u, 1, r], xpeer)

    def fwd_cp(u, r, buf):
        q = lax.rem(tp + 2, 4)
        return rdma(buf.at[q, blk(r)], buf.at[q, blk(r)], fwd.at[u, 0, r], fwd.at[u, 1, r], cpeer)

    def chip_sum(u, r):
        d2d_cp(u, r).wait_recv()
        xs[blk(r), :] = acc[c, 1 - x, blk(r), :] + dd[1 - x, blk(r), :]
        x_cp(u, r).start()

    def total(u, r):
        x_cp(u, r).wait_recv()
        return (acc[c, x, blk(r), :] + dd[x, blk(r), :] + xr[blk(r), :]).astype(BF16)

    def gather(u, r, buf):
        agc_cp(u, r, buf).start()
        agx_cp(u, r, buf).start()

    def relay(u, r, buf):
        agx_cp(u, r, buf).wait_recv()
        fwd_cp(u, r, buf).start()

    def settle(u, buf):
        for r in range(NR):
            agc_cp(u, r, buf).wait_recv()
            fwd_cp(u, r, buf).wait_recv()
        for r in range(NR):
            d2d_cp(u, r).wait_send()
            x_cp(u, r).wait_send()
            agc_cp(u, r, buf).wait_send()
            agx_cp(u, r, buf).wait_send()
            fwd_cp(u, r, buf).wait_send()

    for j in range(8):
        ocopy(j).wait()

    def wo_rows(src, part):
        @pl.loop(0, 8)
        def _(n):
            cols = pl.ds(pl.multiple_of(n * 512, 512), 512)
            v = jnp.dot(src[:, 0:C], dbuf[0, :, cols], preferred_element_type=F32)
            for j in range(1, 8):
                v += jnp.dot(src[:, j * C:(j + 1) * C], dbuf[j, :, cols], preferred_element_type=F32)
            q = n // 2
            acc[lax.rem(q, 2), q // 2, part, pl.ds(pl.multiple_of(lax.rem(n, 2) * 512, 512), 512)] = v

    wo_rows(o_ref, slice(0, 64))
    for r in range(NR // 2):
        d2d_cp(0, r).start()
    for r in range(NR // 2):
        chip_sum(0, r)
    ocp.wait_recv()
    wo_rows(oall, slice(64, 128))
    dcopy0().start()
    for ch in range(1, ND):
        dcopy(ch).start()
    for r in range(NR // 2, NR):
        d2d_cp(0, r).start()
    for r in range(NR // 2, NR):
        chip_sum(0, r)
    qcols = pl.ds(pl.multiple_of(tp * 1024, 1024), 1024)
    sq = []
    for r in range(NR):
        att = total(0, r)
        first = r < NR // 2
        off = (r if first else r - NR // 2) * RB
        rows = pl.ds(pl.multiple_of((dm if first else 1 - dm) * 64 + off, RB), RB)
        h1 = (hid[rows, qcols].astype(F32) + att.astype(F32)).astype(BF16)
        hq[tp, blk(r)] = h1
        gather(0, r, hq)
        h32 = h1.astype(F32)
        sq.append(jnp.sum(h32 * h32, axis=-1, keepdims=True))
    st[flat] = row_to_lanes(jnp.concatenate(sq, axis=0))

    def st_cp(k, own):
        f, dev = at_flat(k)
        if own:
            return rdma(st.at[flat], st.at[flat], stsem.at[0, f], stsem.at[1, flat], dev)
        return rdma(st.at[f], st.at[f], stsem.at[0, f], stsem.at[1, f], dev)

    for k in range(1, 8):
        st_cp(k, True).start()
    for r in range(NR):
        relay(0, r, hq)
    for k in range(1, 8):
        st_cp(k, False).wait_recv()
    tot = jnp.zeros((8, 128), F32)
    for f in range(8):
        v = st[f]
        tot += jnp.where(dm == f // 4, v, pltpu.roll(v, 64, 1))
    scale = lax.rsqrt(lanes_to_row(tot[0:1, :]) / width_full + EPS)
    settle(0, hq)
    for k in range(1, 8):
        st_cp(k, True).wait_send()
    ocp.wait_send()
    for q in range(4):
        for r in range(4):
            rows = slice(32 * r, 32 * r + 32)
            cols = slice(1024 * q, 1024 * q + 1024)
            x2[rows, cols] = (hq[q, rows].astype(F32) * scale[rows, :] * gain[0:1, cols].astype(F32)).astype(BF16)

    def zero_acc():
        for a in range(2):
            for b in range(2):
                acc[a, b] = jnp.zeros((128, 1024), F32)

    zero_acc()

    def g_cp(ch, w=C):
        return rdma(gsnd.at[ch, :, :, 0:w], grcv.at[ch, :, :, 0:w], gs.at[ch], gr.at[ch], ypeer)

    def m_cp(ch, w=C):
        return rdma(mall.at[ch, 0:64, 0:w], mall.at[ch, 64:128, 0:w], ms.at[ch], mr.at[ch], ypeer)

    def up_gate(ch, slot, w=C):
        for t in range(2):
            v = jnp.dot(x2[...], wbuf[slot, t, :, 0:w], preferred_element_type=F32)
            gown[ch, t, :, 0:w] = v[0:64]
            gsnd[ch, t, :, 0:w] = v[64:128]
        g_cp(ch, w).start()

    def act(ch, w=C):
        g_cp(ch, w).wait_recv()
        g = gown[ch, 0, :, 0:w] + grcv[ch, 0, :, 0:w]
        u = gown[ch, 1, :, 0:w] + grcv[ch, 1, :, 0:w]
        mall[ch, 0:64, 0:w] = (g * jax.nn.sigmoid(g) * u).astype(BF16)
        m_cp(ch, w).start()

    def down(ch, slot, w=C):
        m_cp(ch, w).wait_recv()
        m = mall[ch, :, 0:w]

        @pl.loop(0, 4)
        def _(q):
            a, b = lax.rem(q, 2), q // 2
            for n in range(2):
                cols = pl.ds(pl.multiple_of(q * 1024 + n * 512, 512), 512)
                acc[a, b, :, n * 512:(n + 1) * 512] += jnp.dot(m, dbuf[slot, 0:w, cols], preferred_element_type=F32)

    for t in range(2):
        wcopy0(t).wait()
    up_gate(0, 0, 128)
    for t in range(2):
        wcopy(NB, t).start()

    @pl.loop(1, N + DLAG)
    def _(it):
        @pl.when(it < N)
        def _():
            for t in range(2):
                wcopy(it, t).wait()
            up_gate(it, lax.rem(it, NB))

            @pl.when(it + NB < N)
            def _():
                for t in range(2):
                    wcopy(it + NB, t).start()

        @pl.when(it == LAG)
        def _():
            act(0, 128)

        @pl.when((it > LAG) & (it < N + LAG))
        def _():
            act(it - LAG)

        @pl.when(it == DLAG)
        def _():
            dcopy0().wait()
            down(0, 0, 128)
            dcopy(ND).start()

        @pl.when(it > DLAG)
        def _():
            ch = it - DLAG
            dcopy(ch).wait()
            down(ch, dslot(ch))

            @pl.when(ch + ND < N)
            def _():
                dcopy(ch + ND).start()

    for r in range(NR):
        d2d_cp(1, r).start()
    for r in range(NR):
        chip_sum(1, r)
    for r in range(NR):
        mlp = total(1, r)
        oq[tp, blk(r)] = (hq[tp, blk(r)].astype(F32) + mlp.astype(F32)).astype(BF16)
        gather(1, r, oq)
    for r in range(NR):
        relay(1, r, oq)
    settle(1, oq)
    g_cp(0, 128).wait_send()
    m_cp(0, 128).wait_send()

    @pl.loop(1, N)
    def _(ch):
        g_cp(ch).wait_send()
        m_cp(ch).wait_send()

    for q in range(4):
        cols = slice(1024 * q, 1024 * q + 1024)
        out[half(dm), cols] = oq[q, 0:64, :]
        out[half(1 - dm), cols] = oq[q, 64:128, :]


def mlp_call(o, hidden, gain, wo, wg, wu, wd, width_full):
    dma = pltpu.SemaphoreType.DMA
    return pl.pallas_call(
        functools.partial(mlp_kernel, width_full),
        out_shape=jax.ShapeDtypeStruct((128, 4096), BF16),
        in_specs=[VM, VM, VM, ANY, ANY, ANY, ANY], out_specs=VM,
        scratch_shapes=[
            pltpu.VMEM((NB, 2, 4096, C), BF16),
            pltpu.VMEM((ND, C, 4096), BF16),
            pltpu.VMEM((64, 2048), BF16),
            pltpu.VMEM((2, 2, 128, 1024), F32),
            pltpu.VMEM((2, 128, 1024), F32),
            pltpu.VMEM((128, 1024), F32),
            pltpu.VMEM((128, 1024), F32),
            pltpu.VMEM((4, 128, 1024), BF16),
            pltpu.VMEM((4, 128, 1024), BF16),
            pltpu.VMEM((128, 4096), BF16),
            pltpu.VMEM((N, 2, 64, C), F32),
            pltpu.VMEM((N, 2, 64, C), F32),
            pltpu.VMEM((N, 2, 64, C), F32),
            pltpu.VMEM((N, 128, C), BF16),
            pltpu.VMEM((8, 8, 128), F32),
            dma((NB, 2)), dma((ND,)), dma((2,)),
            dma((2, 2, NR)), dma((2, 2, NR)), dma((2, 2, NR)), dma((2, 2, NR)), dma((2, 2, NR)),
            dma((2, 8)), dma((N,)), dma((N,)), dma((N,)), dma((N,)),
        ],
        compiler_params=pltpu.CompilerParams(collective_id=2, has_side_effects=True, vmem_limit_bytes=60 * 2**20),
        name='mlp',
    )(o, hidden, gain, wo, wg, wu, wd)


def solution(mesh):
    width_shards = mesh.shape['dm']
    row_spec = P('dp', 'dm')
    cache_spec = P(('dp', 'dm'), None, 'tp', None)
    batch_spec = P(('dp', 'dm'))
    rope_spec = P(('dp', 'dm'), None)
    in_specs = (row_spec, P('dm', 'tp', None), P('dm', 'tp', None), P('dm', 'tp', None), P('tp', None, 'dm'), P('dm', 'tp'), P('dm', 'tp'), P('tp', 'dm'), P('dm'), P('dm'), cache_spec, cache_spec, batch_spec, rope_spec, rope_spec)
    out_specs = (row_spec, cache_spec, cache_spec)

    def local_layer(hidden, w_q, w_k, w_v, w_o, w_gate, w_up, w_down, norm_attn, norm_mlp, k_cache, v_cache, seq_lens, rope_cos, rope_sin):
        width_full = hidden.shape[1] * width_shards
        x_norm = norm_call(hidden, norm_attn.reshape(1, -1), width_full)
        q_part = jnp.einsum('bd,dhk->hbk', x_norm, w_q, preferred_element_type=F32)
        k_part = jnp.einsum('bd,dhk->hbk', x_norm, w_k, preferred_element_type=F32)
        v_part = jnp.einsum('bd,dhk->hbk', x_norm, w_v, preferred_element_type=F32)
        q_rot, kv_new = rope_call(q_part, jnp.concatenate([k_part, v_part], axis=0), rope_cos, rope_sin)
        k_out, v_out, o = attn_call(q_rot, kv_new, seq_lens, k_cache.reshape(64, 256, 128), v_cache.reshape(64, 256, 128))
        h_out = mlp_call(o, hidden, norm_mlp.reshape(1, -1), w_o.reshape(-1, w_o.shape[-1]), w_gate, w_up, w_down, width_full)
        return h_out, k_out.reshape(k_cache.shape), v_out.reshape(v_cache.shape)

    return jax.shard_map(local_layer, mesh=mesh, in_specs=in_specs, out_specs=out_specs, check_vma=False)
```

```python
import functools

import jax
import jax.numpy as jnp
from jax import lax
from jax.experimental import pallas as pl
from jax.experimental.pallas import tpu as pltpu
from jax.sharding import PartitionSpec as P

EPS = 1e-6
MESH = pl.DeviceIdType.MESH
F32 = jnp.float32
BF16 = jnp.bfloat16
ANY = pl.BlockSpec(memory_space=pl.ANY)
VM = pl.BlockSpec(memory_space=pltpu.VMEM)
HB = pl.BlockSpec(memory_space=pltpu.HBM)
SM = pl.BlockSpec(memory_space=pltpu.SMEM)


def me():
    return lax.axis_index('dp'), lax.axis_index('dm'), lax.axis_index('tp')


def row_to_lanes(col):
    return jnp.broadcast_to(col, (128, 128)).T[0:8, :]


def lanes_to_row(vec):
    return jnp.broadcast_to(vec, (128, 128)).T[:, 0:1]


KC = 8
VLIM = 55
PAIRS = 10


def qkv_kernel(width_full, h_hbm, g_hbm, cos_hbm, sin_hbm, wq, wk, wv, qo_ref, kvo_ref,
               h_ref, g_ref, cos_ref, sin_ref, insem, rawq, rawkv, wall, x_s, part, rbuf, mine_st, their_st, qsem, kvsem, ss, rs, stsem):
    dp, dm, tp = me()
    peer = (dp, 1 - dm, tp)
    mine = pl.ds(pl.multiple_of(dm * 64, 64), 64)
    other = pl.ds(pl.multiple_of((1 - dm) * 64, 64), 64)
    qrows = 65536 // KC

    def kvcopy(t):
        return pltpu.make_async_copy((wk, wv)[t], rawkv.at[t], kvsem.at[t])

    def qcopy(j):
        rows = pl.ds(pl.multiple_of(j * qrows, qrows), qrows)
        return pltpu.make_async_copy(wq.at[rows], rawq.at[rows], qsem.at[j])

    ins = [pltpu.make_async_copy(a, b, insem.at[i]) for i, (a, b) in enumerate(((h_hbm, h_ref), (g_hbm, g_ref), (cos_hbm, cos_ref), (sin_hbm, sin_ref)))]
    for cp in ins:
        cp.start()
    for t in range(2):
        kvcopy(t).start()
    for j in range(KC):
        qcopy(j).start()
    bar = pltpu.get_barrier_semaphore()
    pl.semaphore_signal(bar, inc=1, device_id=peer, device_id_type=MESH)
    ins[0].wait()
    sq = jnp.zeros((128, 128), F32)
    for j in range(32):
        h = h_ref[:, 128 * j:128 * j + 128].astype(F32)
        sq += h * h
    mine_st[...] = row_to_lanes(jnp.sum(sq, axis=-1, keepdims=True))
    pl.semaphore_wait(bar, 1)
    stat = pltpu.make_async_remote_copy(mine_st, their_st, stsem.at[0], stsem.at[1], device_id=peer, device_id_type=MESH)
    stat.start()

    r_i = lax.broadcasted_iota(jnp.int32, (256, 256), 0)
    c_i = lax.broadcasted_iota(jnp.int32, (256, 256), 1)
    perm_kv = jnp.where(c_i == 2 * lax.rem(r_i, 128) + r_i // 128, 1.0, 0.0).astype(BF16)
    for t in range(2):
        kvcopy(t).wait()

    @pl.loop(0, 8)
    def _(j):
        for i in range(4):
            at = pl.ds(pl.multiple_of(j * 1024 + i * 256, 256), 256)
            to = pl.ds(pl.multiple_of(j * 512 + i * 128, 128), 128)
            d = jnp.dot(perm_kv, jnp.concatenate([rawkv[0, at, :], rawkv[1, at, :]], axis=1), preferred_element_type=F32).astype(BF16)
            wall[0, to, :] = d[0:128]
            wall[1, to, :] = d[128:256]

    stat.wait()
    ins[1].wait()
    scale = lax.rsqrt(lanes_to_row(mine_st[0:1, :] + their_st[0:1, :]) / width_full + EPS)
    for j in range(32):
        cols = slice(128 * j, 128 * j + 128)
        x_s[:, cols] = (h_ref[:, cols].astype(F32) * scale * g_ref[j:j + 1, :].astype(F32)).astype(BF16)

    def send(i):
        return pltpu.make_async_remote_copy(part.at[i, other, :], rbuf.at[i], ss.at[i], rs.at[i], device_id=peer, device_id_type=MESH)

    def product(i):
        part[i] = jnp.dot(x_s[...], wall[i], preferred_element_type=F32)
        send(i).start()

    @pl.loop(0, 2)
    def _(i):
        product(i)

    r_h = lax.broadcasted_iota(jnp.int32, (128, 256), 0)
    c_h = lax.broadcasted_iota(jnp.int32, (128, 256), 1)
    for half in range(2):
        perm_q = jnp.where(c_h == 16 * lax.rem(r_h, 16) + r_h // 16 + 8 * half, 1.0, 0.0).astype(BF16)

        @pl.loop(0, KC)
        def _(j):
            if half == 0:
                qcopy(j).wait()
            n = qrows // 512
            for i in range(n):
                a0 = pl.ds(pl.multiple_of(j * qrows + i * 512, 256), 256)
                a1 = pl.ds(pl.multiple_of(j * qrows + i * 512 + 256, 256), 256)
                to = pl.ds(pl.multiple_of((j * n + i) * 32, 32), 32)
                d = jnp.dot(perm_q, jnp.concatenate([rawq[a0, :], rawq[a1, :]], axis=1), preferred_element_type=F32).astype(BF16)
                for h in range(8):
                    rows = slice(16 * h, 16 * h + 16)
                    wall[2 + 4 * half + h // 2, to, (h % 2) * 128:(h % 2) * 128 + 128] = jnp.concatenate([d[rows, 0:128], d[rows, 128:256]], axis=0)

        @pl.loop(2 + 4 * half, 6 + 4 * half)
        def _(i):
            product(i)

    ins[2].wait()
    ins[3].wait()
    c = cos_ref[...]
    s = sin_ref[...]
    cos2 = jnp.concatenate([c, c], axis=-1)
    sin2 = jnp.concatenate([-s, s], axis=-1)

    def rope(a):
        return (a * cos2 + pltpu.roll(a, 64, 1) * sin2).astype(BF16)

    for i in range(PAIRS):
        send(i).wait_recv()
        lo = part[i, mine, 0:128] + rbuf[i, :, 0:128]
        hi = part[i, mine, 128:256] + rbuf[i, :, 128:256]
        if i < 2:
            kvo_ref[i] = rope(lo)
            kvo_ref[2 + i] = hi.astype(BF16)
        else:
            qo_ref[2 * i - 4] = rope(lo)
            qo_ref[2 * i - 3] = rope(hi)
    for i in range(PAIRS):
        send(i).wait_send()


def qkv_call(hidden, gain, cos, sin, wq, wk, wv, width_full):
    dma = pltpu.SemaphoreType.DMA
    return pl.pallas_call(
        functools.partial(qkv_kernel, width_full),
        out_shape=(jax.ShapeDtypeStruct((16, 64, 128), BF16), jax.ShapeDtypeStruct((4, 64, 128), BF16)),
        in_specs=[HB] * 7, out_specs=(VM, VM),
        scratch_shapes=[
            pltpu.VMEM((128, 4096), BF16), pltpu.VMEM((32, 128), BF16), pltpu.VMEM((64, 64), F32), pltpu.VMEM((64, 64), F32), dma((4,)),
            pltpu.VMEM((65536, 128), BF16),
            pltpu.VMEM((2, 8192, 128), BF16),
            pltpu.VMEM((PAIRS, 4096, 256), BF16),
            pltpu.VMEM((128, 4096), BF16),
            pltpu.VMEM((PAIRS, 128, 256), F32),
            pltpu.VMEM((PAIRS, 64, 256), F32),
            pltpu.VMEM((8, 128), F32), pltpu.VMEM((8, 128), F32),
            dma((KC,)), dma((2,)), dma((PAIRS,)), dma((PAIRS,)), dma((2,)),
        ],
        compiler_params=pltpu.CompilerParams(collective_id=0, has_side_effects=True, vmem_limit_bytes=VLIM * 2**20),
        name='qkv',
    )(hidden, gain, cos, sin, wq, wk, wv)


ACH = 4
AROWS = 64 // ACH


def attn_kernel(q_ref, kv_ref, len_ref, kc, vc, ko, vo, o_hbm, kb, vb, qs, os, o_ref, isem, osem, obsem):
    def cin(ch, t):
        rows = pl.ds(ch * AROWS, AROWS)
        return pltpu.make_async_copy((kc, vc)[t].at[rows], (kb, vb)[t].at[rows], isem.at[t, ch])

    def cout(ch, t):
        rows = pl.ds(ch * AROWS, AROWS)
        return pltpu.make_async_copy((kb, vb)[t].at[rows], (ko, vo)[t].at[rows], osem.at[t, ch])

    for ch in range(ACH):
        for t in range(2):
            cin(ch, t).start()
    for h in range(16):
        qs[pl.ds(h, 64, stride=16), :] = q_ref[h].astype(F32)
    row16 = lax.broadcasted_iota(jnp.int32, (16, 128), 0)
    col = lax.broadcasted_iota(jnp.int32, (16, 256), 1)
    head = lax.broadcasted_iota(jnp.int32, (16, 256), 0)
    own = lax.rem(col, 2) == head // 8

    @pl.loop(0, ACH)
    def _(ch):
        cin(ch, 0).wait()
        cin(ch, 1).wait()
        kv32 = [kv_ref[j, pl.ds(pl.multiple_of(ch * AROWS, AROWS), AROWS), :].astype(F32) for j in range(4)]
        for i in range(AROWS):
            b = ch * AROWS + i
            ln = len_ref[b]
            t8 = ln // 8
            at = pl.ds(pl.multiple_of(t8 * 16, 16), 16)
            r0 = 2 * (ln - 8 * t8)
            for t, buf in enumerate((kb, vb)):
                old = buf[b, at, :].astype(F32)
                n0 = jnp.broadcast_to(kv32[2 * t][i:i + 1, :], (16, 128))
                n1 = jnp.broadcast_to(kv32[2 * t + 1][i:i + 1, :], (16, 128))
                new = jnp.where(row16 == r0, n0, jnp.where(row16 == r0 + 1, n1, old))
                buf[b, at, :] = new.astype(BF16)
        cout(ch, 0).start()
        cout(ch, 1).start()
        sc = []
        for i in range(AROWS):
            b = ch * AROWS + i
            q = qs[pl.ds(pl.multiple_of(b * 16, 16), 16), :].astype(BF16)
            sc.append(lax.dot_general(q, kb[b], (((1,), (1,)), ((), ())), preferred_element_type=F32))
        pr = []
        for i in range(AROWS):
            ln = len_ref[ch * AROWS + i]
            s = jnp.where(own & (col <= 2 * ln + 1), sc[i] * (128.0 ** -0.5), -1e30)
            p = jnp.exp(s - jnp.max(s, axis=-1, keepdims=True))
            pr.append((p / jnp.sum(p, axis=-1, keepdims=True)).astype(BF16))
        for i in range(AROWS):
            b = ch * AROWS + i
            os[pl.ds(pl.multiple_of(b * 16, 16), 16), :] = jnp.dot(pr[i], vb[b], preferred_element_type=F32)

    for h in range(16):
        o_ref[:, h * 128:(h + 1) * 128] = os[pl.ds(h, 64, stride=16), :].astype(BF16)
    ocp = pltpu.make_async_copy(o_ref, o_hbm, obsem)
    ocp.start()
    for ch in range(ACH):
        cout(ch, 0).wait()
        cout(ch, 1).wait()
    ocp.wait()


def attn_call(q_rot, kv_new, seq_lens, k_cache, v_cache):
    cache = jax.ShapeDtypeStruct((64, 256, 128), BF16)
    return pl.pallas_call(
        attn_kernel,
        out_shape=(cache, cache, jax.ShapeDtypeStruct((64, 2048), BF16)),
        in_specs=[VM, VM, SM, ANY, ANY], out_specs=(ANY, ANY, HB),
        scratch_shapes=[pltpu.VMEM((64, 256, 128), BF16), pltpu.VMEM((64, 256, 128), BF16), pltpu.VMEM((1024, 128), F32), pltpu.VMEM((1024, 128), F32), pltpu.VMEM((64, 2048), BF16),
                        pltpu.SemaphoreType.DMA((2, ACH)), pltpu.SemaphoreType.DMA((2, ACH)), pltpu.SemaphoreType.DMA],
        compiler_params=pltpu.CompilerParams(vmem_limit_bytes=32 * 2**20),
        name='attend',
    )(q_rot, kv_new, seq_lens, k_cache, v_cache)


C = 256
N = 22
NB = 4
ND = 8
NR = 4
RB = 128 // NR
LEAD = 5
LAG = 2
DLAG = 5


def mlp_kernel(width_full, o_hbm, hid_hbm, gain_hbm, wo, wg, wu, wd, out,
               o_ref, hid, gain, insem, wbuf, dbuf, oall, acc, dd, xs, xr, hq, oq, x2, gown, gsnd, grcv, mall, st,
               wsem, dsem, osem, d2d, xx, agc, agx, fwd, stsem, gs, gr, ms, mr):
    dp, dm, tp = me()
    x = tp // 2
    c = lax.rem(tp, 2)
    ypeer = (dp, 1 - dm, tp)
    cpeer = (dp, dm, x * 2 + 1 - c)
    xpeer = (dp, dm, (1 - x) * 2 + c)
    flat = dm * 4 + tp

    def at_flat(k):
        f = lax.rem(flat + k, 8)
        return f, (dp, f // 4, lax.rem(f, 4))

    def rdma(src, dst, s, r, dev):
        return pltpu.make_async_remote_copy(src, dst, s, r, device_id=dev, device_id_type=MESH)

    def blk(r):
        return slice(r * RB, (r + 1) * RB)

    def rows_of(r):
        return pl.ds(pl.multiple_of((dm if r % 2 == 0 else 1 - dm) * 64 + (r // 2) * RB, RB), RB)

    def bchunk(t):
        return jnp.where(t < N - LEAD, t + LEAD, t - (N - LEAD))

    BODD = 2 * N - LEAD

    def col(ch):
        return pl.multiple_of(ch * C - 128, 128)

    def wcopy(s, ch, t):
        slot = lax.rem(s, NB)
        return pltpu.make_async_copy((wg, wu)[t].at[:, pl.ds(col(ch), C)], wbuf.at[slot, t], wsem.at[slot, t])

    def wcopy0(s, t):
        slot = s % NB
        return pltpu.make_async_copy((wg, wu)[t].at[:, 0:128], wbuf.at[slot, t, :, 0:128], wsem.at[slot, t])

    def opiece(n):
        return (1 - x) * 4 + n if n < 4 else x * 4 + n - 4

    def ocopy(n):
        cols = pl.ds(pl.multiple_of(opiece(n) * 512, 512), 512)
        return pltpu.make_async_copy(wo.at[:, :, cols], dbuf.at[:, :, cols], dsem.at[n])

    def dcopy(d, ch):
        slot = lax.rem(d, ND)
        return pltpu.make_async_copy(wd.at[pl.ds(col(ch), C)], dbuf.at[slot], dsem.at[slot])

    def dcopy0(d):
        slot = d % ND
        return pltpu.make_async_copy(wd.at[0:128], dbuf.at[slot, 0:128], dsem.at[slot])

    ins = [pltpu.make_async_copy(a, b, insem.at[i]) for i, (a, b) in enumerate(((o_hbm, o_ref), (hid_hbm, hid), (gain_hbm, gain)))]
    ins[0].start()
    for j in range(8):
        ocopy(j).start()
    ins[1].start()
    ins[2].start()

    bar = pltpu.get_barrier_semaphore()
    for k in range(1, 8):
        pl.semaphore_signal(bar, inc=1, device_id=at_flat(k)[1], device_id_type=MESH)
    pl.semaphore_wait(bar, 7)

    def ocp(b):
        return rdma(o_ref.at[blk(b)], oall.at[blk(b)], osem.at[0, b], osem.at[1, b], ypeer)

    ins[0].wait()
    ocp(0).start()
    ocp(1).start()

    def d2d_cp(u, p, r):
        xq = 1 - x if p == 0 else x
        return rdma(acc.at[1 - c, xq, blk(r), :], dd.at[xq, blk(r), :], d2d.at[u, p, 0, r], d2d.at[u, p, 1, r], cpeer)

    def x_cp(u, r):
        return rdma(xs.at[blk(r)], xr.at[blk(r)], xx.at[u, 0, r], xx.at[u, 1, r], xpeer)

    def agc_cp(u, r, buf):
        return rdma(buf.at[tp, blk(r)], buf.at[tp, blk(r)], agc.at[u, 0, r], agc.at[u, 1, r], cpeer)

    def agx_cp(u, r, buf):
        return rdma(buf.at[tp, blk(r)], buf.at[tp, blk(r)], agx.at[u, 0, r], agx.at[u, 1, r], xpeer)

    def fwd_cp(u, r, buf):
        q = lax.rem(tp + 2, 4)
        return rdma(buf.at[q, blk(r)], buf.at[q, blk(r)], fwd.at[u, 0, r], fwd.at[u, 1, r], cpeer)

    def chip_sum(u, r):
        d2d_cp(u, 0, r).wait_recv()
        xs[blk(r), :] = acc[c, 1 - x, blk(r), :] + dd[1 - x, blk(r), :]
        x_cp(u, r).start()

    def total(u, r):
        d2d_cp(u, 1, r).wait_recv()
        x_cp(u, r).wait_recv()
        return (acc[c, x, blk(r), :] + dd[x, blk(r), :] + xr[blk(r), :]).astype(BF16)

    def gather(u, r, buf):
        agx_cp(u, r, buf).start()
        agc_cp(u, r, buf).start()

    def relay(u, r, buf):
        agx_cp(u, r, buf).wait_recv()
        fwd_cp(u, r, buf).start()

    def arrived(u, r, buf):
        agc_cp(u, r, buf).wait_recv()
        fwd_cp(u, r, buf).wait_recv()

    def drained(u, r, buf):
        d2d_cp(u, 0, r).wait_send()
        d2d_cp(u, 1, r).wait_send()
        x_cp(u, r).wait_send()
        agc_cp(u, r, buf).wait_send()
        agx_cp(u, r, buf).wait_send()
        fwd_cp(u, r, buf).wait_send()

    def zero_acc():
        for a in range(2):
            for b in range(2):
                acc[a, b] = jnp.zeros((128, 1024), F32)

    def acc_cols(n):
        q = n // 2
        return q % 2, q // 2, slice((n % 2) * 512, (n % 2) * 512 + 512)

    def wo_piece(src, n, rs):
        at = opiece(n)
        cols = pl.ds(pl.multiple_of(at * 512, 512), 512)
        v = jnp.dot(src[:, 0:C], dbuf[0, :, cols], preferred_element_type=F32)
        for j in range(1, 8):
            v += jnp.dot(src[:, j * C:(j + 1) * C], dbuf[j, :, cols], preferred_element_type=F32)
        q = at // 2
        for i, r in enumerate(rs):
            acc[lax.rem(q, 2), q // 2, blk(r), (n % 2) * 512:(n % 2) * 512 + 512] = v[i * RB:i * RB + RB]

    def own(ns):
        for n in ns:
            ocopy(n).wait()
            wo_piece(o_ref, n, (0, 2))

    def peers(r, ns):
        for n in ns:
            wo_piece(oall.at[blk(r // 2)], n, (r,))

    own(range(4))
    d2d_cp(0, 0, 0).start()
    d2d_cp(0, 0, 2).start()
    own((4, 5))
    chip_sum(0, 0)
    own((6, 7))
    d2d_cp(0, 1, 0).start()
    d2d_cp(0, 1, 2).start()
    for t in range(2):
        wcopy0(0, t).start()
    for s in range(1, NB):
        for t in range(2):
            wcopy(s, s, t).start()
    ocp(0).wait_recv()
    peers(1, range(4))
    d2d_cp(0, 0, 1).start()
    peers(1, (4, 5))
    chip_sum(0, 1)
    peers(1, (6, 7))
    d2d_cp(0, 1, 1).start()
    ins[1].wait()
    ins[2].wait()
    qcols = pl.ds(pl.multiple_of(tp * 1024, 1024), 1024)

    def h_mid(r):
        att = total(0, r)
        h1 = (hid[rows_of(r), qcols].astype(F32) + att.astype(F32)).astype(BF16)
        hq[tp, blk(r)] = h1
        gather(0, r, hq)
        h32 = h1.astype(F32)
        return jnp.sum(h32 * h32, axis=-1, keepdims=True)

    def st_cp(b, k, own):
        f, dev = at_flat(k)
        if own:
            return rdma(st.at[b, flat], st.at[b, flat], stsem.at[b, 0, f], stsem.at[b, 1, flat], dev)
        return rdma(st.at[b, f], st.at[b, f], stsem.at[b, 0, f], stsem.at[b, 1, f], dev)

    def stats(b, sq):
        st[b, flat] = row_to_lanes(jnp.concatenate(sq + [jnp.zeros((64, 1), F32)], axis=0))
        for k in range(1, 8):
            st_cp(b, k, True).start()

    lane = lax.broadcasted_iota(jnp.int32, (8, 128), 1)

    def x2_rows(b):
        for k in range(1, 8):
            st_cp(b, k, False).wait_recv()
        tot = jnp.zeros((8, 128), F32)
        for f in range(8):
            v = st[b, f]
            swapped = jnp.where(lane < RB, pltpu.roll(v, 128 - RB, 1), pltpu.roll(v, RB, 1))
            tot += jnp.where(dm == f // 4, v, swapped)
        scale = lax.rsqrt(lanes_to_row(tot[0:1, :]) / width_full + EPS)[0:64]
        rows = slice(64 * b, 64 * b + 64)
        arrived(0, 2 * b, hq)
        arrived(0, 2 * b + 1, hq)
        for j in range(32):
            x2[rows, 128 * j:128 * j + 128] = (hq[j // 8, rows, 128 * (j % 8):128 * (j % 8) + 128].astype(F32) * scale * gain[j:j + 1, :].astype(F32)).astype(BF16)

    sq0 = h_mid(0)
    ocp(1).wait_recv()
    peers(3, range(4))
    d2d_cp(0, 0, 3).start()
    peers(3, (4, 5))
    stats(0, [sq0, h_mid(1)])
    chip_sum(0, 2)
    peers(3, (6, 7))
    d2d_cp(0, 1, 3).start()
    dcopy0(0).start()
    for d in range(1, ND):
        dcopy(d, d).start()
    relay(0, 0, hq)
    chip_sum(0, 3)
    relay(0, 1, hq)
    x2_rows(0)

    def g_cp(b, ch, w=C):
        return rdma(gsnd.at[b, ch, :, :, 0:w], grcv.at[b, ch, :, :, 0:w], gs.at[b, ch], gr.at[b, ch], ypeer)

    def m_cp(b, ch, w=C):
        return rdma(mall.at[b, ch, 0:RB, 0:w], mall.at[b, ch, RB:2 * RB, 0:w], ms.at[b, ch], mr.at[b, ch], ypeer)

    def up_gate(ch, slot, blocks, w=C):
        lo, hi = blocks[0] * 64, blocks[-1] * 64 + 64
        for t in range(2):
            v = jnp.dot(x2[lo:hi, :], wbuf[slot, t, :, 0:w], preferred_element_type=F32)
            for i, b in enumerate(blocks):
                gown[b, ch, t, :, 0:w] = v[64 * i:64 * i + RB]
                gsnd[b, ch, t, :, 0:w] = v[64 * i + RB:64 * i + 64]

    def act(b, ch, w=C):
        g_cp(b, ch, w).wait_recv()
        g = gown[b, ch, 0, :, 0:w] + grcv[b, ch, 0, :, 0:w]
        u = gown[b, ch, 1, :, 0:w] + grcv[b, ch, 1, :, 0:w]
        mall[b, ch, 0:RB, 0:w] = (g * jax.nn.sigmoid(g) * u).astype(BF16)
        m_cp(b, ch, w).start()

    def down(b, ch, slot, w=C):
        m_cp(b, ch, w).wait_recv()
        m = mall[b, ch, :, 0:w]
        rows = pl.ds(pl.multiple_of(b * 64, 64), 64)

        for n in range(8):
            a, bb, cols = acc_cols(n)
            acc[a, bb, rows, cols] += jnp.dot(m, dbuf[slot, 0:w, n * 512:n * 512 + 512], preferred_element_type=F32)

    sqb = []

    def second_half(step):
        if step == 0:
            sqb.append(h_mid(2))
        elif step == 2:
            sqb.append(h_mid(3))
            stats(1, sqb)
        elif step == 3:
            relay(0, 2, hq)
            relay(0, 3, hq)
        elif step == LEAD - 1:
            x2_rows(1)
            for r in range(NR):
                drained(0, r, hq)
            zero_acc()

    for e in range(LEAD):
        for t in range(2):
            (wcopy0(0, t) if e == 0 else wcopy(e, e, t)).wait()
        up_gate(e, e % NB, [0], 128 if e == 0 else C)
        g_cp(0, e, 128 if e == 0 else C).start()
        for t in range(2):
            wcopy(e + NB, e + NB, t).start()
        if e >= LAG:
            act(0, e - LAG, 128 if e == LAG else C)
        second_half(e)

    def split(e):
        b = e // N
        return b, jnp.where(b == 0, e, bchunk(e - N))

    @pl.loop(LEAD, 2 * N + DLAG)
    def _(e):
        @pl.when(e < N)
        def _():
            for t in range(2):
                wcopy(e, e, t).wait()
            up_gate(e, lax.rem(e, NB), [0, 1])

        @pl.when(e == N)
        def _():
            for t in range(2):
                wcopy0(N, t).wait()
            up_gate(0, N % NB, [1], 128)

        @pl.when((e > N) & (e < N + LEAD))
        def _():
            for t in range(2):
                wcopy(e, e - N, t).wait()
            up_gate(e - N, lax.rem(e, NB), [1])

        @pl.when((e < 2 * N) & (e != BODD))
        def _():
            b, ch = split(e)
            g_cp(b, ch).start()

        @pl.when(e == BODD)
        def _():
            g_cp(1, 0, 128).start()

        s = e + NB

        @pl.when((s < N + LEAD) & (s != N))
        def _():
            for t in range(2):
                wcopy(s, jnp.where(s < N, s, s - N), t).start()

        @pl.when(s == N)
        def _():
            for t in range(2):
                wcopy0(N, t).start()

        i = e - LAG

        @pl.when((i < 2 * N) & (i != BODD))
        def _():
            b, ch = split(i)
            act(b, ch)

        @pl.when(i == BODD)
        def _():
            act(1, 0, 128)

        d = e - DLAG

        @pl.when(d == 0)
        def _():
            dcopy0(0).wait()
            down(0, 0, 0, 128)

        @pl.when(d == BODD)
        def _():
            dcopy0(BODD).wait()
            down(1, 0, BODD % ND, 128)

        @pl.when((d > 0) & (d != BODD))
        def _():
            b, ch = split(d)
            dcopy(d, ch).wait()
            down(b, ch, lax.rem(d, ND))

        f = d + ND

        @pl.when((f < 2 * N) & (f != BODD))
        def _():
            dcopy(f, split(f)[1]).start()

        @pl.when(f == BODD)
        def _():
            dcopy0(BODD).start()

        def res(r):
            mlp = total(1, r)
            oq[tp, blk(r)] = (hq[tp, blk(r)].astype(F32) + mlp.astype(F32)).astype(BF16)
            gather(1, r, oq)

        @pl.when(d == N)
        def _():
            for r in (0, 1):
                d2d_cp(1, 0, r).start()
                d2d_cp(1, 1, r).start()

        @pl.when(d == N + 1)
        def _():
            chip_sum(1, 0)
            chip_sum(1, 1)

        @pl.when(d == N + 5)
        def _():
            res(0)

        @pl.when(d == N + 7)
        def _():
            res(1)

        @pl.when(d == N + 10)
        def _():
            relay(1, 0, oq)
            relay(1, 1, oq)

    for r in (2, 3):
        d2d_cp(1, 0, r).start()
    for r in (2, 3):
        d2d_cp(1, 1, r).start()
    for r in (2, 3):
        chip_sum(1, r)
    for r in (2, 3):
        mlp = total(1, r)
        oq[tp, blk(r)] = (hq[tp, blk(r)].astype(F32) + mlp.astype(F32)).astype(BF16)
        gather(1, r, oq)
    for r in (2, 3):
        relay(1, r, oq)
    for b in range(2):
        for k in range(1, 8):
            st_cp(b, k, True).wait_send()
        ocp(b).wait_send()
        g_cp(b, 0, 128).wait_send()
        m_cp(b, 0, 128).wait_send()

    @pl.loop(1, N)
    def _(ch):
        for b in range(2):
            g_cp(b, ch).wait_send()
            m_cp(b, ch).wait_send()

    for r in range(NR):
        arrived(1, r, oq)
        for q in range(4):
            out[rows_of(r), 1024 * q:1024 * q + 1024] = oq[q, blk(r), :]
    for r in range(NR):
        drained(1, r, oq)


def mlp_call(o, hidden, gain, wo, wg, wu, wd, width_full):
    dma = pltpu.SemaphoreType.DMA
    return pl.pallas_call(
        functools.partial(mlp_kernel, width_full),
        out_shape=jax.ShapeDtypeStruct((128, 4096), BF16),
        in_specs=[HB] * 7, out_specs=VM,
        scratch_shapes=[
            pltpu.VMEM((64, 2048), BF16), pltpu.VMEM((128, 4096), BF16), pltpu.VMEM((32, 128), BF16), dma((3,)),
            pltpu.VMEM((NB, 2, 4096, C), BF16),
            pltpu.VMEM((ND, C, 4096), BF16),
            pltpu.VMEM((64, 2048), BF16),
            pltpu.VMEM((2, 2, 128, 1024), F32),
            pltpu.VMEM((2, 128, 1024), F32),
            pltpu.VMEM((128, 1024), F32),
            pltpu.VMEM((128, 1024), F32),
            pltpu.VMEM((4, 128, 1024), BF16),
            pltpu.VMEM((4, 128, 1024), BF16),
            pltpu.VMEM((128, 4096), BF16),
            pltpu.VMEM((2, N, 2, RB, C), F32),
            pltpu.VMEM((2, N, 2, RB, C), F32),
            pltpu.VMEM((2, N, 2, RB, C), F32),
            pltpu.VMEM((2, N, 2 * RB, C), BF16),
            pltpu.VMEM((2, 8, 8, 128), F32),
            dma((NB, 2)), dma((ND,)), dma((2, 2)),
            dma((2, 2, 2, NR)), dma((2, 2, NR)), dma((2, 2, NR)), dma((2, 2, NR)), dma((2, 2, NR)),
            dma((2, 2, 8)), dma((2, N)), dma((2, N)), dma((2, N)), dma((2, N)),
        ],
        compiler_params=pltpu.CompilerParams(collective_id=2, has_side_effects=True, vmem_limit_bytes=56 * 2**20),
        name='mlp',
    )(o, hidden, gain, wo, wg, wu, wd)


def solution(mesh):
    width_shards = mesh.shape['dm']
    row_spec = P('dp', 'dm')
    cache_spec = P(('dp', 'dm'), None, 'tp', None)
    batch_spec = P(('dp', 'dm'))
    rope_spec = P(('dp', 'dm'), None)
    in_specs = (row_spec, P('dm', 'tp', None), P('dm', 'tp', None), P('dm', 'tp', None), P('tp', None, 'dm'), P('dm', 'tp'), P('dm', 'tp'), P('tp', 'dm'), P('dm'), P('dm'), cache_spec, cache_spec, batch_spec, rope_spec, rope_spec)
    out_specs = (row_spec, cache_spec, cache_spec)

    def local_layer(hidden, w_q, w_k, w_v, w_o, w_gate, w_up, w_down, norm_attn, norm_mlp, k_cache, v_cache, seq_lens, rope_cos, rope_sin):
        width_full = hidden.shape[1] * width_shards
        q_rot, kv_new = qkv_call(hidden, norm_attn.reshape(-1, 128), rope_cos, rope_sin, w_q.reshape(-1, 128), w_k.reshape(-1, 128), w_v.reshape(-1, 128), width_full)
        k_out, v_out, o = attn_call(q_rot, kv_new, seq_lens, k_cache.reshape(64, 256, 128), v_cache.reshape(64, 256, 128))
        h_out = mlp_call(o, hidden, norm_mlp.reshape(-1, 128), w_o.reshape(8, 256, -1), w_gate, w_up, w_down, width_full)
        return h_out, k_out.reshape(k_cache.shape), v_out.reshape(v_cache.shape)

    return jax.shard_map(local_layer, mesh=mesh, in_specs=in_specs, out_specs=out_specs, check_vma=False)
```

```python
import functools

import jax
import jax.numpy as jnp
from jax import lax
from jax.experimental import pallas as pl
from jax.experimental.pallas import tpu as pltpu
from jax.sharding import PartitionSpec as P

EPS = 1e-6
MESH = pl.DeviceIdType.MESH
F32 = jnp.float32
BF16 = jnp.bfloat16
ANY = pl.BlockSpec(memory_space=pl.ANY)
VM = pl.BlockSpec(memory_space=pltpu.VMEM)
HB = pl.BlockSpec(memory_space=pltpu.HBM)
SM = pl.BlockSpec(memory_space=pltpu.SMEM)


def me():
    return lax.axis_index('dp'), lax.axis_index('dm'), lax.axis_index('tp')


def row_to_lanes(col):
    return jnp.broadcast_to(col, (128, 128)).T[0:8, :]


def lanes_to_row(vec):
    return jnp.broadcast_to(vec, (128, 128)).T[:, 0:1]


KC = 4
VLIM = 60
PAIRS = 10


def qkv_kernel(width_full, h_hbm, g_hbm, cos_hbm, sin_hbm, wq, wk, wv, qo_ref, kvo_ref,
               h_ref, g_ref, cos_ref, sin_ref, insem, rawq, rawkv, wall, x_s, part, rbuf, mine_st, their_st, qsem, kvsem, ss, rs, stsem):
    dp, dm, tp = me()
    peer = (dp, 1 - dm, tp)
    mine = pl.ds(pl.multiple_of(dm * 64, 64), 64)
    other = pl.ds(pl.multiple_of((1 - dm) * 64, 64), 64)
    qrows = 65536 // KC

    def kvcopy(t):
        return pltpu.make_async_copy((wk, wv)[t], rawkv.at[t], kvsem.at[t])

    def qcopy(j):
        rows = pl.ds(pl.multiple_of(j * qrows, qrows), qrows)
        return pltpu.make_async_copy(wq.at[rows], rawq.at[rows], qsem.at[j])

    ins = [pltpu.make_async_copy(a, b, insem.at[i]) for i, (a, b) in enumerate(((h_hbm, h_ref), (g_hbm, g_ref), (cos_hbm, cos_ref), (sin_hbm, sin_ref)))]
    for cp in ins:
        cp.start()
    for t in range(2):
        kvcopy(t).start()
    for j in range(KC):
        qcopy(j).start()
    bar = pltpu.get_barrier_semaphore()
    pl.semaphore_signal(bar, inc=1, device_id=peer, device_id_type=MESH)
    ins[0].wait()
    sq = jnp.zeros((128, 128), F32)
    for j in range(32):
        h = h_ref[:, 128 * j:128 * j + 128].astype(F32)
        sq += h * h
    mine_st[...] = row_to_lanes(jnp.sum(sq, axis=-1, keepdims=True))
    pl.semaphore_wait(bar, 1)
    stat = pltpu.make_async_remote_copy(mine_st, their_st, stsem.at[0], stsem.at[1], device_id=peer, device_id_type=MESH)
    stat.start()

    r_i = lax.broadcasted_iota(jnp.int32, (256, 256), 0)
    c_i = lax.broadcasted_iota(jnp.int32, (256, 256), 1)
    perm_kv = jnp.where(c_i == 2 * lax.rem(r_i, 128) + r_i // 128, 1.0, 0.0).astype(BF16)
    for t in range(2):
        kvcopy(t).wait()

    @pl.loop(0, 8)
    def _(j):
        for i in range(4):
            at = pl.ds(pl.multiple_of(j * 1024 + i * 256, 256), 256)
            to = pl.ds(pl.multiple_of(j * 512 + i * 128, 128), 128)
            d = jnp.dot(perm_kv, jnp.concatenate([rawkv[0, at, :], rawkv[1, at, :]], axis=1), preferred_element_type=F32).astype(BF16)
            wall[0, to, :] = d[0:128]
            wall[1, to, :] = d[128:256]

    stat.wait()
    ins[1].wait()
    scale = lax.rsqrt(lanes_to_row(mine_st[0:1, :] + their_st[0:1, :]) / width_full + EPS)
    for j in range(32):
        cols = slice(128 * j, 128 * j + 128)
        x_s[:, cols] = (h_ref[:, cols].astype(F32) * scale * g_ref[j:j + 1, :].astype(F32)).astype(BF16)

    def send(i):
        return pltpu.make_async_remote_copy(part.at[i, other, :], rbuf.at[i], ss.at[i], rs.at[i], device_id=peer, device_id_type=MESH)

    def products(i):
        for k in range(2):
            part[i + k] = jnp.dot(x_s[...], wall[i + k], preferred_element_type=F32)
        for k in range(2):
            send(i + k).start()

    products(0)

    r_h = lax.broadcasted_iota(jnp.int32, (128, 256), 0)
    c_h = lax.broadcasted_iota(jnp.int32, (128, 256), 1)
    for half in range(2):
        perm_q = jnp.where(c_h == 16 * lax.rem(r_h, 16) + r_h // 16 + 8 * half, 1.0, 0.0).astype(BF16)

        @pl.loop(0, KC)
        def _(j):
            if half == 0:
                qcopy(j).wait()
            n = qrows // 512
            for i in range(n):
                a0 = pl.ds(pl.multiple_of(j * qrows + i * 512, 256), 256)
                a1 = pl.ds(pl.multiple_of(j * qrows + i * 512 + 256, 256), 256)
                to = pl.ds(pl.multiple_of((j * n + i) * 32, 32), 32)
                d = jnp.dot(perm_q, jnp.concatenate([rawq[a0, :], rawq[a1, :]], axis=1), preferred_element_type=F32).astype(BF16)
                for h in range(8):
                    rows = slice(16 * h, 16 * h + 16)
                    wall[2 + 4 * half + h // 2, to, (h % 2) * 128:(h % 2) * 128 + 128] = jnp.concatenate([d[rows, 0:128], d[rows, 128:256]], axis=0)

        products(2 + 4 * half)
        products(4 + 4 * half)

    ins[2].wait()
    ins[3].wait()
    c = cos_ref[...]
    s = sin_ref[...]
    cos2 = jnp.concatenate([c, c], axis=-1)
    sin2 = jnp.concatenate([-s, s], axis=-1)

    def rope(a):
        return (a * cos2 + pltpu.roll(a, 64, 1) * sin2).astype(BF16)

    for i in range(PAIRS):
        send(i).wait_recv()
        lo = part[i, mine, 0:128] + rbuf[i, :, 0:128]
        hi = part[i, mine, 128:256] + rbuf[i, :, 128:256]
        if i < 2:
            kvo_ref[i] = rope(lo)
            kvo_ref[2 + i] = hi.astype(BF16)
        else:
            qo_ref[2 * i - 4] = rope(lo)
            qo_ref[2 * i - 3] = rope(hi)
    for i in range(PAIRS):
        send(i).wait_send()


def qkv_call(hidden, gain, cos, sin, wq, wk, wv, width_full):
    dma = pltpu.SemaphoreType.DMA
    return pl.pallas_call(
        functools.partial(qkv_kernel, width_full),
        out_shape=(jax.ShapeDtypeStruct((16, 64, 128), BF16), jax.ShapeDtypeStruct((4, 64, 128), BF16)),
        in_specs=[HB] * 7, out_specs=(VM, VM),
        scratch_shapes=[
            pltpu.VMEM((128, 4096), BF16), pltpu.VMEM((32, 128), BF16), pltpu.VMEM((64, 64), F32), pltpu.VMEM((64, 64), F32), dma((4,)),
            pltpu.VMEM((65536, 128), BF16),
            pltpu.VMEM((2, 8192, 128), BF16),
            pltpu.VMEM((PAIRS, 4096, 256), BF16),
            pltpu.VMEM((128, 4096), BF16),
            pltpu.VMEM((PAIRS, 128, 256), F32),
            pltpu.VMEM((PAIRS, 64, 256), F32),
            pltpu.VMEM((8, 128), F32), pltpu.VMEM((8, 128), F32),
            dma((KC,)), dma((2,)), dma((PAIRS,)), dma((PAIRS,)), dma((2,)),
        ],
        compiler_params=pltpu.CompilerParams(collective_id=0, has_side_effects=True, vmem_limit_bytes=VLIM * 2**20),
        name='qkv',
    )(hidden, gain, cos, sin, wq, wk, wv)


ACH = 4
AROWS = 64 // ACH


def attn_kernel(q_hbm, kv_hbm, len_ref, kc, vc, ko, vo, o_hbm, kb, vb, qs, os, o_ref, q_ref, kv_ref, isem, osem, obsem, qsem):
    def cin(ch, t):
        rows = pl.ds(ch * AROWS, AROWS)
        return pltpu.make_async_copy((kc, vc)[t].at[rows], (kb, vb)[t].at[rows], isem.at[t, ch])

    def cout(ch, t):
        rows = pl.ds(ch * AROWS, AROWS)
        return pltpu.make_async_copy((kb, vb)[t].at[rows], (ko, vo)[t].at[rows], osem.at[t, ch])

    ins = [pltpu.make_async_copy(q_hbm, q_ref, qsem.at[0]), pltpu.make_async_copy(kv_hbm, kv_ref, qsem.at[1])]
    for cp in ins:
        cp.start()
    for ch in range(ACH):
        for t in range(2):
            cin(ch, t).start()
    for cp in ins:
        cp.wait()
    for h in range(16):
        qs[pl.ds(h, 64, stride=16), :] = q_ref[h].astype(F32)
    row16 = lax.broadcasted_iota(jnp.int32, (16, 128), 0)
    col = lax.broadcasted_iota(jnp.int32, (16, 256), 1)
    head = lax.broadcasted_iota(jnp.int32, (16, 256), 0)
    own = lax.rem(col, 2) == head // 8

    @pl.loop(0, ACH)
    def _(ch):
        cin(ch, 0).wait()
        cin(ch, 1).wait()
        kv32 = [kv_ref[j, pl.ds(pl.multiple_of(ch * AROWS, AROWS), AROWS), :].astype(F32) for j in range(4)]
        for i in range(AROWS):
            b = ch * AROWS + i
            ln = len_ref[b]
            t8 = ln // 8
            at = pl.ds(pl.multiple_of(t8 * 16, 16), 16)
            r0 = 2 * (ln - 8 * t8)
            for t, buf in enumerate((kb, vb)):
                old = buf[b, at, :].astype(F32)
                n0 = jnp.broadcast_to(kv32[2 * t][i:i + 1, :], (16, 128))
                n1 = jnp.broadcast_to(kv32[2 * t + 1][i:i + 1, :], (16, 128))
                new = jnp.where(row16 == r0, n0, jnp.where(row16 == r0 + 1, n1, old))
                buf[b, at, :] = new.astype(BF16)
        cout(ch, 0).start()
        cout(ch, 1).start()
        sc = []
        for i in range(AROWS):
            b = ch * AROWS + i
            q = qs[pl.ds(pl.multiple_of(b * 16, 16), 16), :].astype(BF16)
            sc.append(lax.dot_general(q, kb[b], (((1,), (1,)), ((), ())), preferred_element_type=F32))
        pr = []
        for i in range(AROWS):
            ln = len_ref[ch * AROWS + i]
            s = jnp.where(own & (col <= 2 * ln + 1), sc[i] * (128.0 ** -0.5), -1e30)
            p = jnp.exp(s - jnp.max(s, axis=-1, keepdims=True))
            pr.append((p / jnp.sum(p, axis=-1, keepdims=True)).astype(BF16))
        for i in range(AROWS):
            b = ch * AROWS + i
            os[pl.ds(pl.multiple_of(b * 16, 16), 16), :] = jnp.dot(pr[i], vb[b], preferred_element_type=F32)

    for h in range(16):
        o_ref[:, h * 128:(h + 1) * 128] = os[pl.ds(h, 64, stride=16), :].astype(BF16)
    ocp = pltpu.make_async_copy(o_ref, o_hbm, obsem)
    ocp.start()
    for ch in range(ACH):
        cout(ch, 0).wait()
        cout(ch, 1).wait()
    ocp.wait()


def attn_call(q_rot, kv_new, seq_lens, k_cache, v_cache):
    cache = jax.ShapeDtypeStruct((64, 256, 128), BF16)
    return pl.pallas_call(
        attn_kernel,
        out_shape=(cache, cache, jax.ShapeDtypeStruct((64, 2048), BF16)),
        in_specs=[HB, HB, SM, HB, HB], out_specs=(HB, HB, HB),
        scratch_shapes=[pltpu.VMEM((64, 256, 128), BF16), pltpu.VMEM((64, 256, 128), BF16), pltpu.VMEM((1024, 128), F32), pltpu.VMEM((1024, 128), F32), pltpu.VMEM((64, 2048), BF16),
                        pltpu.VMEM((16, 64, 128), BF16), pltpu.VMEM((4, 64, 128), BF16),
                        pltpu.SemaphoreType.DMA((2, ACH)), pltpu.SemaphoreType.DMA((2, ACH)), pltpu.SemaphoreType.DMA, pltpu.SemaphoreType.DMA((2,))],
        compiler_params=pltpu.CompilerParams(vmem_limit_bytes=60 * 2**20),
        name='attend',
    )(q_rot, kv_new, seq_lens, k_cache, v_cache)


C = 256
N = 22
NB = 4
ND = 8
NR = 4
RB = 128 // NR
LEAD = 5
LAG = 2
DLAG = 5


def mlp_kernel(width_full, o_hbm, hid_hbm, gain_hbm, wo, wg, wu, wd, out,
               o_ref, hid, gain, insem, wbuf, dbuf, oall, acc, dd, xs, xr, hq, oq, x2, gown, gsnd, grcv, mall, st,
               wsem, dsem, osem, d2d, xx, agc, agx, fwd, stsem, gs, gr, ms, mr):
    dp, dm, tp = me()
    x = tp // 2
    c = lax.rem(tp, 2)
    ypeer = (dp, 1 - dm, tp)
    cpeer = (dp, dm, x * 2 + 1 - c)
    xpeer = (dp, dm, (1 - x) * 2 + c)
    flat = dm * 4 + tp

    def at_flat(k):
        f = lax.rem(flat + k, 8)
        return f, (dp, f // 4, lax.rem(f, 4))

    def rdma(src, dst, s, r, dev):
        return pltpu.make_async_remote_copy(src, dst, s, r, device_id=dev, device_id_type=MESH)

    def blk(r):
        return slice(r * RB, (r + 1) * RB)

    def rows_of(r):
        return pl.ds(pl.multiple_of((dm if r % 2 == 0 else 1 - dm) * 64 + (r // 2) * RB, RB), RB)

    def bchunk(t):
        return jnp.where(t < N - LEAD, t + LEAD, t - (N - LEAD))

    BODD = 2 * N - LEAD

    def col(ch):
        return pl.multiple_of(ch * C - 128, 128)

    def wcopy(s, ch, t):
        slot = lax.rem(s, NB)
        return pltpu.make_async_copy((wg, wu)[t].at[:, pl.ds(col(ch), C)], wbuf.at[slot, t], wsem.at[slot, t])

    def wcopy0(s, t):
        slot = s % NB
        return pltpu.make_async_copy((wg, wu)[t].at[:, 0:128], wbuf.at[slot, t, :, 0:128], wsem.at[slot, t])

    def opiece(n):
        return (1 - x) * 4 + n if n < 4 else x * 4 + n - 4

    def ocopy(n):
        cols = pl.ds(pl.multiple_of(opiece(n) * 512, 512), 512)
        return pltpu.make_async_copy(wo.at[:, :, cols], dbuf.at[:, :, cols], dsem.at[n])

    def dcopy(d, ch):
        slot = lax.rem(d, ND)
        return pltpu.make_async_copy(wd.at[pl.ds(col(ch), C)], dbuf.at[slot], dsem.at[slot])

    def dcopy0(d):
        slot = d % ND
        return pltpu.make_async_copy(wd.at[0:128], dbuf.at[slot, 0:128], dsem.at[slot])

    ins = [pltpu.make_async_copy(a, b, insem.at[i]) for i, (a, b) in enumerate(((o_hbm, o_ref), (hid_hbm, hid), (gain_hbm, gain)))]
    ins[0].start()
    for j in range(8):
        ocopy(j).start()
    ins[1].start()
    ins[2].start()

    bar = pltpu.get_barrier_semaphore()
    for k in range(1, 8):
        pl.semaphore_signal(bar, inc=1, device_id=at_flat(k)[1], device_id_type=MESH)
    pl.semaphore_wait(bar, 7)

    def ocp(b):
        return rdma(o_ref.at[blk(b)], oall.at[blk(b)], osem.at[0, b], osem.at[1, b], ypeer)

    ins[0].wait()
    ocp(0).start()
    ocp(1).start()

    def d2d_cp(u, p, r):
        xq = 1 - x if p == 0 else x
        return rdma(acc.at[1 - c, xq, blk(r), :], dd.at[xq, blk(r), :], d2d.at[u, p, 0, r], d2d.at[u, p, 1, r], cpeer)

    def x_cp(u, r):
        return rdma(xs.at[blk(r)], xr.at[blk(r)], xx.at[u, 0, r], xx.at[u, 1, r], xpeer)

    def agc_cp(u, r, buf):
        return rdma(buf.at[tp, blk(r)], buf.at[tp, blk(r)], agc.at[u, 0, r], agc.at[u, 1, r], cpeer)

    def agx_cp(u, r, buf):
        return rdma(buf.at[tp, blk(r)], buf.at[tp, blk(r)], agx.at[u, 0, r], agx.at[u, 1, r], xpeer)

    def fwd_cp(u, r, buf):
        q = lax.rem(tp + 2, 4)
        return rdma(buf.at[q, blk(r)], buf.at[q, blk(r)], fwd.at[u, 0, r], fwd.at[u, 1, r], cpeer)

    def chip_sum(u, r):
        d2d_cp(u, 0, r).wait_recv()
        xs[blk(r), :] = acc[c, 1 - x, blk(r), :] + dd[1 - x, blk(r), :]
        x_cp(u, r).start()

    def total(u, r):
        d2d_cp(u, 1, r).wait_recv()
        x_cp(u, r).wait_recv()
        return (acc[c, x, blk(r), :] + dd[x, blk(r), :] + xr[blk(r), :]).astype(BF16)

    def gather(u, r, buf):
        agx_cp(u, r, buf).start()
        agc_cp(u, r, buf).start()

    def relay(u, r, buf):
        agx_cp(u, r, buf).wait_recv()
        fwd_cp(u, r, buf).start()

    def arrived(u, r, buf):
        agc_cp(u, r, buf).wait_recv()
        fwd_cp(u, r, buf).wait_recv()

    def drained(u, r, buf):
        d2d_cp(u, 0, r).wait_send()
        d2d_cp(u, 1, r).wait_send()
        x_cp(u, r).wait_send()
        agc_cp(u, r, buf).wait_send()
        agx_cp(u, r, buf).wait_send()
        fwd_cp(u, r, buf).wait_send()

    def zero_acc():
        for a in range(2):
            for b in range(2):
                acc[a, b] = jnp.zeros((128, 1024), F32)

    def acc_cols(n):
        q = n // 2
        return q % 2, q // 2, slice((n % 2) * 512, (n % 2) * 512 + 512)

    def wo_piece(src, n, rs):
        at = opiece(n)
        cols = pl.ds(pl.multiple_of(at * 512, 512), 512)
        v = jnp.dot(src[:, 0:C], dbuf[0, :, cols], preferred_element_type=F32)
        for j in range(1, 8):
            v += jnp.dot(src[:, j * C:(j + 1) * C], dbuf[j, :, cols], preferred_element_type=F32)
        q = at // 2
        for i, r in enumerate(rs):
            acc[lax.rem(q, 2), q // 2, blk(r), (n % 2) * 512:(n % 2) * 512 + 512] = v[i * RB:i * RB + RB]

    def own(ns):
        for n in ns:
            ocopy(n).wait()
            wo_piece(o_ref, n, (0, 2))

    def peers(r, ns):
        for n in ns:
            wo_piece(oall.at[blk(r // 2)], n, (r,))

    own(range(4))
    d2d_cp(0, 0, 0).start()
    d2d_cp(0, 0, 2).start()
    own((4, 5))
    chip_sum(0, 0)
    own((6, 7))
    d2d_cp(0, 1, 0).start()
    d2d_cp(0, 1, 2).start()
    for t in range(2):
        wcopy0(0, t).start()
    for s in range(1, NB):
        for t in range(2):
            wcopy(s, s, t).start()
    ocp(0).wait_recv()
    peers(1, range(4))
    d2d_cp(0, 0, 1).start()
    peers(1, (4, 5))
    chip_sum(0, 1)
    peers(1, (6, 7))
    d2d_cp(0, 1, 1).start()
    ins[1].wait()
    ins[2].wait()
    qcols = pl.ds(pl.multiple_of(tp * 1024, 1024), 1024)

    def h_mid(r):
        att = total(0, r)
        h1 = (hid[rows_of(r), qcols].astype(F32) + att.astype(F32)).astype(BF16)
        hq[tp, blk(r)] = h1
        gather(0, r, hq)
        h32 = h1.astype(F32)
        return jnp.sum(h32 * h32, axis=-1, keepdims=True)

    def st_cp(b, k, own):
        f, dev = at_flat(k)
        if own:
            return rdma(st.at[b, flat], st.at[b, flat], stsem.at[b, 0, f], stsem.at[b, 1, flat], dev)
        return rdma(st.at[b, f], st.at[b, f], stsem.at[b, 0, f], stsem.at[b, 1, f], dev)

    def stats(b, sq):
        st[b, flat] = row_to_lanes(jnp.concatenate(sq + [jnp.zeros((64, 1), F32)], axis=0))
        for k in range(1, 8):
            st_cp(b, k, True).start()

    lane = lax.broadcasted_iota(jnp.int32, (8, 128), 1)

    def x2_rows(b):
        for k in range(1, 8):
            st_cp(b, k, False).wait_recv()
        tot = jnp.zeros((8, 128), F32)
        for f in range(8):
            v = st[b, f]
            swapped = jnp.where(lane < RB, pltpu.roll(v, 128 - RB, 1), pltpu.roll(v, RB, 1))
            tot += jnp.where(dm == f // 4, v, swapped)
        scale = lax.rsqrt(lanes_to_row(tot[0:1, :]) / width_full + EPS)[0:64]
        rows = slice(64 * b, 64 * b + 64)
        arrived(0, 2 * b, hq)
        arrived(0, 2 * b + 1, hq)
        for j in range(32):
            x2[rows, 128 * j:128 * j + 128] = (hq[j // 8, rows, 128 * (j % 8):128 * (j % 8) + 128].astype(F32) * scale * gain[j:j + 1, :].astype(F32)).astype(BF16)

    sq0 = h_mid(0)
    ocp(1).wait_recv()
    peers(3, range(4))
    d2d_cp(0, 0, 3).start()
    peers(3, (4, 5))
    stats(0, [sq0, h_mid(1)])
    chip_sum(0, 2)
    peers(3, (6, 7))
    d2d_cp(0, 1, 3).start()
    dcopy0(0).start()
    for d in range(1, ND):
        dcopy(d, d).start()
    relay(0, 0, hq)
    chip_sum(0, 3)
    relay(0, 1, hq)
    x2_rows(0)

    def g_cp(b, ch, w=C):
        return rdma(gsnd.at[b, ch, :, :, 0:w], grcv.at[b, ch, :, :, 0:w], gs.at[b, ch], gr.at[b, ch], ypeer)

    def m_cp(b, ch, w=C):
        return rdma(mall.at[b, ch, 0:RB, 0:w], mall.at[b, ch, RB:2 * RB, 0:w], ms.at[b, ch], mr.at[b, ch], ypeer)

    def up_gate(ch, slot, blocks, w=C):
        lo, hi = blocks[0] * 64, blocks[-1] * 64 + 64
        for t in range(2):
            v = jnp.dot(x2[lo:hi, :], wbuf[slot, t, :, 0:w], preferred_element_type=F32)
            for i, b in enumerate(blocks):
                gown[b, ch, t, :, 0:w] = v[64 * i:64 * i + RB]
                gsnd[b, ch, t, :, 0:w] = v[64 * i + RB:64 * i + 64]

    def act(b, ch, w=C):
        g_cp(b, ch, w).wait_recv()
        g = gown[b, ch, 0, :, 0:w] + grcv[b, ch, 0, :, 0:w]
        u = gown[b, ch, 1, :, 0:w] + grcv[b, ch, 1, :, 0:w]
        mall[b, ch, 0:RB, 0:w] = (g * jax.nn.sigmoid(g) * u).astype(BF16)
        m_cp(b, ch, w).start()

    def down(b, ch, slot, w=C):
        m_cp(b, ch, w).wait_recv()
        m = mall[b, ch, :, 0:w]
        rows = pl.ds(pl.multiple_of(b * 64, 64), 64)

        for n in range(8):
            a, bb, cols = acc_cols(n)
            acc[a, bb, rows, cols] += jnp.dot(m, dbuf[slot, 0:w, n * 512:n * 512 + 512], preferred_element_type=F32)

    sqb = []

    def second_half(step):
        if step == 0:
            sqb.append(h_mid(2))
        elif step == 2:
            sqb.append(h_mid(3))
            stats(1, sqb)
        elif step == 3:
            relay(0, 2, hq)
            relay(0, 3, hq)
        elif step == LEAD - 1:
            x2_rows(1)
            for r in range(NR):
                drained(0, r, hq)
            zero_acc()

    for e in range(LEAD):
        for t in range(2):
            (wcopy0(0, t) if e == 0 else wcopy(e, e, t)).wait()
        up_gate(e, e % NB, [0], 128 if e == 0 else C)
        g_cp(0, e, 128 if e == 0 else C).start()
        for t in range(2):
            wcopy(e + NB, e + NB, t).start()
        if e >= LAG:
            act(0, e - LAG, 128 if e == LAG else C)
        second_half(e)

    def split(e):
        b = e // N
        return b, jnp.where(b == 0, e, bchunk(e - N))

    @pl.loop(LEAD, 2 * N + DLAG)
    def _(e):
        @pl.when(e < N)
        def _():
            for t in range(2):
                wcopy(e, e, t).wait()
            up_gate(e, lax.rem(e, NB), [0, 1])

        @pl.when(e == N)
        def _():
            for t in range(2):
                wcopy0(N, t).wait()
            up_gate(0, N % NB, [1], 128)

        @pl.when((e > N) & (e < N + LEAD))
        def _():
            for t in range(2):
                wcopy(e, e - N, t).wait()
            up_gate(e - N, lax.rem(e, NB), [1])

        @pl.when((e < 2 * N) & (e != BODD))
        def _():
            b, ch = split(e)
            g_cp(b, ch).start()

        @pl.when(e == BODD)
        def _():
            g_cp(1, 0, 128).start()

        s = e + NB

        @pl.when((s < N + LEAD) & (s != N))
        def _():
            for t in range(2):
                wcopy(s, jnp.where(s < N, s, s - N), t).start()

        @pl.when(s == N)
        def _():
            for t in range(2):
                wcopy0(N, t).start()

        i = e - LAG

        @pl.when((i < 2 * N) & (i != BODD))
        def _():
            b, ch = split(i)
            act(b, ch)

        @pl.when(i == BODD)
        def _():
            act(1, 0, 128)

        d = e - DLAG

        @pl.when(d == 0)
        def _():
            dcopy0(0).wait()
            down(0, 0, 0, 128)

        @pl.when(d == BODD)
        def _():
            dcopy0(BODD).wait()
            down(1, 0, BODD % ND, 128)

        @pl.when((d > 0) & (d != BODD))
        def _():
            b, ch = split(d)
            dcopy(d, ch).wait()
            down(b, ch, lax.rem(d, ND))

        f = d + ND

        @pl.when((f < 2 * N) & (f != BODD))
        def _():
            dcopy(f, split(f)[1]).start()

        @pl.when(f == BODD)
        def _():
            dcopy0(BODD).start()

        def res(r):
            mlp = total(1, r)
            oq[tp, blk(r)] = (hq[tp, blk(r)].astype(F32) + mlp.astype(F32)).astype(BF16)
            gather(1, r, oq)

        @pl.when(d == N)
        def _():
            for r in (0, 1):
                d2d_cp(1, 0, r).start()
                d2d_cp(1, 1, r).start()

        @pl.when(d == N + 1)
        def _():
            chip_sum(1, 0)
            chip_sum(1, 1)

        @pl.when(d == N + 5)
        def _():
            res(0)

        @pl.when(d == N + 7)
        def _():
            res(1)

        @pl.when(d == N + 10)
        def _():
            relay(1, 0, oq)
            relay(1, 1, oq)

    for r in (2, 3):
        d2d_cp(1, 0, r).start()
    for r in (2, 3):
        d2d_cp(1, 1, r).start()
    for r in (2, 3):
        chip_sum(1, r)
    for r in (2, 3):
        mlp = total(1, r)
        oq[tp, blk(r)] = (hq[tp, blk(r)].astype(F32) + mlp.astype(F32)).astype(BF16)
        gather(1, r, oq)
    for r in (2, 3):
        relay(1, r, oq)
    for b in range(2):
        for k in range(1, 8):
            st_cp(b, k, True).wait_send()
        ocp(b).wait_send()
        g_cp(b, 0, 128).wait_send()
        m_cp(b, 0, 128).wait_send()

    @pl.loop(1, N)
    def _(ch):
        for b in range(2):
            g_cp(b, ch).wait_send()
            m_cp(b, ch).wait_send()

    for r in range(NR):
        arrived(1, r, oq)
        for q in range(4):
            out[rows_of(r), 1024 * q:1024 * q + 1024] = oq[q, blk(r), :]
    for r in range(NR):
        drained(1, r, oq)


def mlp_call(o, hidden, gain, wo, wg, wu, wd, width_full):
    dma = pltpu.SemaphoreType.DMA
    return pl.pallas_call(
        functools.partial(mlp_kernel, width_full),
        out_shape=jax.ShapeDtypeStruct((128, 4096), BF16),
        in_specs=[HB] * 7, out_specs=VM,
        scratch_shapes=[
            pltpu.VMEM((64, 2048), BF16), pltpu.VMEM((128, 4096), BF16), pltpu.VMEM((32, 128), BF16), dma((3,)),
            pltpu.VMEM((NB, 2, 4096, C), BF16),
            pltpu.VMEM((ND, C, 4096), BF16),
            pltpu.VMEM((64, 2048), BF16),
            pltpu.VMEM((2, 2, 128, 1024), F32),
            pltpu.VMEM((2, 128, 1024), F32),
            pltpu.VMEM((128, 1024), F32),
            pltpu.VMEM((128, 1024), F32),
            pltpu.VMEM((4, 128, 1024), BF16),
            pltpu.VMEM((4, 128, 1024), BF16),
            pltpu.VMEM((128, 4096), BF16),
            pltpu.VMEM((2, N, 2, RB, C), F32),
            pltpu.VMEM((2, N, 2, RB, C), F32),
            pltpu.VMEM((2, N, 2, RB, C), F32),
            pltpu.VMEM((2, N, 2 * RB, C), BF16),
            pltpu.VMEM((2, 8, 8, 128), F32),
            dma((NB, 2)), dma((ND,)), dma((2, 2)),
            dma((2, 2, 2, NR)), dma((2, 2, NR)), dma((2, 2, NR)), dma((2, 2, NR)), dma((2, 2, NR)),
            dma((2, 2, 8)), dma((2, N)), dma((2, N)), dma((2, N)), dma((2, N)),
        ],
        compiler_params=pltpu.CompilerParams(collective_id=2, has_side_effects=True, vmem_limit_bytes=56 * 2**20),
        name='mlp',
    )(o, hidden, gain, wo, wg, wu, wd)


def solution(mesh):
    width_shards = mesh.shape['dm']
    row_spec = P('dp', 'dm')
    cache_spec = P(('dp', 'dm'), None, 'tp', None)
    batch_spec = P(('dp', 'dm'))
    rope_spec = P(('dp', 'dm'), None)
    in_specs = (row_spec, P('dm', 'tp', None), P('dm', 'tp', None), P('dm', 'tp', None), P('tp', None, 'dm'), P('dm', 'tp'), P('dm', 'tp'), P('tp', 'dm'), P('dm'), P('dm'), cache_spec, cache_spec, batch_spec, rope_spec, rope_spec)
    out_specs = (row_spec, cache_spec, cache_spec)

    def local_layer(hidden, w_q, w_k, w_v, w_o, w_gate, w_up, w_down, norm_attn, norm_mlp, k_cache, v_cache, seq_lens, rope_cos, rope_sin):
        width_full = hidden.shape[1] * width_shards
        q_rot, kv_new = qkv_call(hidden, norm_attn.reshape(-1, 128), rope_cos, rope_sin, w_q.reshape(-1, 128), w_k.reshape(-1, 128), w_v.reshape(-1, 128), width_full)
        k_out, v_out, o = attn_call(q_rot, kv_new, seq_lens, k_cache.reshape(64, 256, 128), v_cache.reshape(64, 256, 128))
        h_out = mlp_call(o, hidden, norm_mlp.reshape(-1, 128), w_o.reshape(8, 256, -1), w_gate, w_up, w_down, width_full)
        return h_out, k_out.reshape(k_cache.shape), v_out.reshape(v_cache.shape)

    return jax.shard_map(local_layer, mesh=mesh, in_specs=in_specs, out_specs=out_specs, check_vma=False)
```

```python
import functools

import jax
import jax.numpy as jnp
from jax import lax
from jax.experimental import pallas as pl
from jax.experimental.pallas import tpu as pltpu
from jax.sharding import PartitionSpec as P

EPS = 1e-6
MESH = pl.DeviceIdType.MESH
F32 = jnp.float32
BF16 = jnp.bfloat16
ANY = pl.BlockSpec(memory_space=pl.ANY)
VM = pl.BlockSpec(memory_space=pltpu.VMEM)
HB = pl.BlockSpec(memory_space=pltpu.HBM)
SM = pl.BlockSpec(memory_space=pltpu.SMEM)


def me():
    return lax.axis_index('dp'), lax.axis_index('dm'), lax.axis_index('tp')


def row_to_lanes(col):
    return jnp.broadcast_to(col, (128, 128)).T[0:8, :]


def lanes_to_row(vec):
    return jnp.broadcast_to(vec, (128, 128)).T[:, 0:1]


KC = 4
VLIM = 60
PAIRS = 10


def qkv_kernel(width_full, h_hbm, g_hbm, cos_hbm, sin_hbm, wq, wk, wv, qo_ref, kvo_ref,
               h_ref, g_ref, cos_ref, sin_ref, insem, rawq, rawkv, wall, x_s, part, rbuf, mine_st, their_st, qsem, kvsem, ss, rs, stsem):
    dp, dm, tp = me()
    peer = (dp, 1 - dm, tp)
    mine = pl.ds(pl.multiple_of(dm * 64, 64), 64)
    other = pl.ds(pl.multiple_of((1 - dm) * 64, 64), 64)
    qrows = 65536 // KC

    def kvcopy(t):
        return pltpu.make_async_copy((wk, wv)[t], rawkv.at[t], kvsem.at[t])

    def qcopy(j):
        rows = pl.ds(pl.multiple_of(j * qrows, qrows), qrows)
        return pltpu.make_async_copy(wq.at[rows], rawq.at[rows], qsem.at[j])

    ins = [pltpu.make_async_copy(a, b, insem.at[i]) for i, (a, b) in enumerate(((h_hbm, h_ref), (g_hbm, g_ref), (cos_hbm, cos_ref), (sin_hbm, sin_ref)))]
    for cp in ins:
        cp.start()
    for t in range(2):
        kvcopy(t).start()
    for j in range(KC):
        qcopy(j).start()
    bar = pltpu.get_barrier_semaphore()
    pl.semaphore_signal(bar, inc=1, device_id=peer, device_id_type=MESH)
    ins[0].wait()
    sq = jnp.zeros((128, 128), F32)
    for j in range(32):
        h = h_ref[:, 128 * j:128 * j + 128].astype(F32)
        sq += h * h
    mine_st[...] = row_to_lanes(jnp.sum(sq, axis=-1, keepdims=True))
    pl.semaphore_wait(bar, 1)
    stat = pltpu.make_async_remote_copy(mine_st, their_st, stsem.at[0], stsem.at[1], device_id=peer, device_id_type=MESH)
    stat.start()

    r_i = lax.broadcasted_iota(jnp.int32, (256, 256), 0)
    c_i = lax.broadcasted_iota(jnp.int32, (256, 256), 1)
    perm_kv = jnp.where(c_i == 2 * lax.rem(r_i, 128) + r_i // 128, 1.0, 0.0).astype(BF16)
    for t in range(2):
        kvcopy(t).wait()

    @pl.loop(0, 8)
    def _(j):
        for i in range(4):
            at = pl.ds(pl.multiple_of(j * 1024 + i * 256, 256), 256)
            to = pl.ds(pl.multiple_of(j * 512 + i * 128, 128), 128)
            d = jnp.dot(perm_kv, jnp.concatenate([rawkv[0, at, :], rawkv[1, at, :]], axis=1), preferred_element_type=F32).astype(BF16)
            wall[0, to, :] = d[0:128]
            wall[1, to, :] = d[128:256]

    stat.wait()
    ins[1].wait()
    scale = lax.rsqrt(lanes_to_row(mine_st[0:1, :] + their_st[0:1, :]) / width_full + EPS)
    for j in range(32):
        cols = slice(128 * j, 128 * j + 128)
        x_s[:, cols] = (h_ref[:, cols].astype(F32) * scale * g_ref[j:j + 1, :].astype(F32)).astype(BF16)

    def send(i):
        return pltpu.make_async_remote_copy(part.at[i, other, :], rbuf.at[i], ss.at[i], rs.at[i], device_id=peer, device_id_type=MESH)

    def products(i):
        for k in range(2):
            part[i + k] = jnp.dot(x_s[...], wall[i + k], preferred_element_type=F32)
        for k in range(2):
            send(i + k).start()

    products(0)

    r_h = lax.broadcasted_iota(jnp.int32, (128, 256), 0)
    c_h = lax.broadcasted_iota(jnp.int32, (128, 256), 1)
    for half in range(2):
        perm_q = jnp.where(c_h == 16 * lax.rem(r_h, 16) + r_h // 16 + 8 * half, 1.0, 0.0).astype(BF16)

        @pl.loop(0, KC)
        def _(j):
            if half == 0:
                qcopy(j).wait()
            n = qrows // 512
            for i in range(n):
                a0 = pl.ds(pl.multiple_of(j * qrows + i * 512, 256), 256)
                a1 = pl.ds(pl.multiple_of(j * qrows + i * 512 + 256, 256), 256)
                to = pl.ds(pl.multiple_of((j * n + i) * 32, 32), 32)
                d = jnp.dot(perm_q, jnp.concatenate([rawq[a0, :], rawq[a1, :]], axis=1), preferred_element_type=F32).astype(BF16)
                for h in range(8):
                    rows = slice(16 * h, 16 * h + 16)
                    wall[2 + 4 * half + h // 2, to, (h % 2) * 128:(h % 2) * 128 + 128] = jnp.concatenate([d[rows, 0:128], d[rows, 128:256]], axis=0)

        products(2 + 4 * half)
        products(4 + 4 * half)

    ins[2].wait()
    ins[3].wait()
    c = cos_ref[...]
    s = sin_ref[...]
    cos2 = jnp.concatenate([c, c], axis=-1)
    sin2 = jnp.concatenate([-s, s], axis=-1)

    def rope(a):
        return (a * cos2 + pltpu.roll(a, 64, 1) * sin2).astype(BF16)

    for i in range(PAIRS):
        send(i).wait_recv()
        lo = part[i, mine, 0:128] + rbuf[i, :, 0:128]
        hi = part[i, mine, 128:256] + rbuf[i, :, 128:256]
        if i < 2:
            kvo_ref[i] = rope(lo)
            kvo_ref[2 + i] = hi.astype(BF16)
        else:
            qo_ref[2 * i - 4] = rope(lo)
            qo_ref[2 * i - 3] = rope(hi)
    for i in range(PAIRS):
        send(i).wait_send()


def qkv_call(hidden, gain, cos, sin, wq, wk, wv, width_full):
    dma = pltpu.SemaphoreType.DMA
    return pl.pallas_call(
        functools.partial(qkv_kernel, width_full),
        out_shape=(jax.ShapeDtypeStruct((16, 64, 128), BF16), jax.ShapeDtypeStruct((4, 64, 128), BF16)),
        in_specs=[HB] * 7, out_specs=(VM, VM),
        scratch_shapes=[
            pltpu.VMEM((128, 4096), BF16), pltpu.VMEM((32, 128), BF16), pltpu.VMEM((64, 64), F32), pltpu.VMEM((64, 64), F32), dma((4,)),
            pltpu.VMEM((65536, 128), BF16),
            pltpu.VMEM((2, 8192, 128), BF16),
            pltpu.VMEM((PAIRS, 4096, 256), BF16),
            pltpu.VMEM((128, 4096), BF16),
            pltpu.VMEM((PAIRS, 128, 256), F32),
            pltpu.VMEM((PAIRS, 64, 256), F32),
            pltpu.VMEM((8, 128), F32), pltpu.VMEM((8, 128), F32),
            dma((KC,)), dma((2,)), dma((PAIRS,)), dma((PAIRS,)), dma((2,)),
        ],
        compiler_params=pltpu.CompilerParams(collective_id=0, has_side_effects=True, vmem_limit_bytes=VLIM * 2**20),
        name='qkv',
    )(hidden, gain, cos, sin, wq, wk, wv)


ACH = 2
AROWS = 64 // ACH


def attn_kernel(q_hbm, kv_hbm, len_ref, kc, vc, ko, vo, o_hbm, kb, vb, qs, os, o_ref, q_ref, kv_ref, isem, osem, obsem, qsem):
    def cin(ch, t):
        rows = pl.ds(ch * AROWS, AROWS)
        return pltpu.make_async_copy((kc, vc)[t].at[rows], (kb, vb)[t].at[rows], isem.at[t, ch])

    def cout(ch, t):
        rows = pl.ds(ch * AROWS, AROWS)
        return pltpu.make_async_copy((kb, vb)[t].at[rows], (ko, vo)[t].at[rows], osem.at[t, ch])

    ins = [pltpu.make_async_copy(q_hbm, q_ref, qsem.at[0]), pltpu.make_async_copy(kv_hbm, kv_ref, qsem.at[1])]
    for cp in ins:
        cp.start()
    for ch in range(ACH):
        for t in range(2):
            cin(ch, t).start()
    for cp in ins:
        cp.wait()
    for h in range(16):
        qs[pl.ds(h, 64, stride=16), :] = q_ref[h].astype(F32)
    row16 = lax.broadcasted_iota(jnp.int32, (16, 128), 0)
    col = lax.broadcasted_iota(jnp.int32, (16, 256), 1)
    head = lax.broadcasted_iota(jnp.int32, (16, 256), 0)
    own = lax.rem(col, 2) == head // 8

    @pl.loop(0, ACH)
    def _(ch):
        cin(ch, 0).wait()
        cin(ch, 1).wait()
        kv32 = [kv_ref[j, pl.ds(pl.multiple_of(ch * AROWS, AROWS), AROWS), :].astype(F32) for j in range(4)]
        for i in range(AROWS):
            b = ch * AROWS + i
            ln = len_ref[b]
            t8 = ln // 8
            at = pl.ds(pl.multiple_of(t8 * 16, 16), 16)
            r0 = 2 * (ln - 8 * t8)
            for t, buf in enumerate((kb, vb)):
                old = buf[b, at, :].astype(F32)
                n0 = jnp.broadcast_to(kv32[2 * t][i:i + 1, :], (16, 128))
                n1 = jnp.broadcast_to(kv32[2 * t + 1][i:i + 1, :], (16, 128))
                new = jnp.where(row16 == r0, n0, jnp.where(row16 == r0 + 1, n1, old))
                buf[b, at, :] = new.astype(BF16)
        cout(ch, 0).start()
        cout(ch, 1).start()
        sc = []
        for i in range(AROWS):
            b = ch * AROWS + i
            q = qs[pl.ds(pl.multiple_of(b * 16, 16), 16), :].astype(BF16)
            sc.append(lax.dot_general(q, kb[b], (((1,), (1,)), ((), ())), preferred_element_type=F32))
        pr = []
        for i in range(AROWS):
            ln = len_ref[ch * AROWS + i]
            s = jnp.where(own & (col <= 2 * ln + 1), sc[i] * (128.0 ** -0.5), -1e30)
            p = jnp.exp(s - jnp.max(s, axis=-1, keepdims=True))
            pr.append((p / jnp.sum(p, axis=-1, keepdims=True)).astype(BF16))
        for i in range(AROWS):
            b = ch * AROWS + i
            os[pl.ds(pl.multiple_of(b * 16, 16), 16), :] = jnp.dot(pr[i], vb[b], preferred_element_type=F32)

    for h in range(16):
        o_ref[:, h * 128:(h + 1) * 128] = os[pl.ds(h, 64, stride=16), :].astype(BF16)
    ocp = pltpu.make_async_copy(o_ref, o_hbm, obsem)
    ocp.start()
    for ch in range(ACH):
        cout(ch, 0).wait()
        cout(ch, 1).wait()
    ocp.wait()


def attn_call(q_rot, kv_new, seq_lens, k_cache, v_cache):
    cache = jax.ShapeDtypeStruct((64, 256, 128), BF16)
    return pl.pallas_call(
        attn_kernel,
        out_shape=(cache, cache, jax.ShapeDtypeStruct((64, 2048), BF16)),
        in_specs=[HB, HB, SM, HB, HB], out_specs=(HB, HB, HB),
        scratch_shapes=[pltpu.VMEM((64, 256, 128), BF16), pltpu.VMEM((64, 256, 128), BF16), pltpu.VMEM((1024, 128), F32), pltpu.VMEM((1024, 128), F32), pltpu.VMEM((64, 2048), BF16),
                        pltpu.VMEM((16, 64, 128), BF16), pltpu.VMEM((4, 64, 128), BF16),
                        pltpu.SemaphoreType.DMA((2, ACH)), pltpu.SemaphoreType.DMA((2, ACH)), pltpu.SemaphoreType.DMA, pltpu.SemaphoreType.DMA((2,))],
        compiler_params=pltpu.CompilerParams(vmem_limit_bytes=60 * 2**20),
        name='attend',
    )(q_rot, kv_new, seq_lens, k_cache, v_cache)


C = 256
N = 22
NB = 4
ND = 8
NR = 4
RB = 128 // NR
LEAD = 6
LAG = 2
DLAG = 6


def mlp_kernel(width_full, o_hbm, hid_hbm, gain_hbm, wo, wg, wu, wd, out,
               o_ref, hid, gain, insem, outv, outsem, wbuf, dbuf, oall, acc, dd, xs, xr, hq, oq, x2, gown, gsnd, grcv, mall, st,
               wsem, dsem, osem, d2d, xx, agc, agx, fwd, stsem, gs, gr, ms, mr):
    dp, dm, tp = me()
    x = tp // 2
    c = lax.rem(tp, 2)
    ypeer = (dp, 1 - dm, tp)
    cpeer = (dp, dm, x * 2 + 1 - c)
    xpeer = (dp, dm, (1 - x) * 2 + c)
    flat = dm * 4 + tp

    def at_flat(k):
        f = lax.rem(flat + k, 8)
        return f, (dp, f // 4, lax.rem(f, 4))

    def rdma(src, dst, s, r, dev):
        return pltpu.make_async_remote_copy(src, dst, s, r, device_id=dev, device_id_type=MESH)

    def blk(r):
        return slice(r * RB, (r + 1) * RB)

    def rows_of(r):
        return pl.ds(pl.multiple_of((dm if r % 2 == 0 else 1 - dm) * 64 + (r // 2) * RB, RB), RB)

    def bchunk(t):
        return jnp.where(t < N - LEAD, t + LEAD, t - (N - LEAD))

    BODD = 2 * N - LEAD

    def col(ch):
        return pl.multiple_of(ch * C - 128, 128)

    def wcopy(s, ch, t):
        slot = lax.rem(s, NB)
        return pltpu.make_async_copy((wg, wu)[t].at[:, pl.ds(col(ch), C)], wbuf.at[slot, t], wsem.at[slot, t])

    def wcopy0(s, t):
        slot = s % NB
        return pltpu.make_async_copy((wg, wu)[t].at[:, 0:128], wbuf.at[slot, t, :, 0:128], wsem.at[slot, t])

    def opiece(n):
        return (1 - x) * 4 + n if n < 4 else x * 4 + n - 4

    def ocopy(n):
        cols = pl.ds(pl.multiple_of(opiece(n) * 512, 512), 512)
        return pltpu.make_async_copy(wo.at[:, :, cols], dbuf.at[:, :, cols], dsem.at[n])

    def dcopy(d, ch):
        slot = lax.rem(d, ND)
        return pltpu.make_async_copy(wd.at[pl.ds(col(ch), C)], dbuf.at[slot], dsem.at[slot])

    def dcopy0(d):
        slot = d % ND
        return pltpu.make_async_copy(wd.at[0:128], dbuf.at[slot, 0:128], dsem.at[slot])

    ins = [pltpu.make_async_copy(a, b, insem.at[i]) for i, (a, b) in enumerate(((o_hbm, o_ref), (hid_hbm, hid), (gain_hbm, gain)))]
    ins[0].start()
    for j in range(8):
        ocopy(j).start()
    ins[1].start()
    ins[2].start()

    bar = pltpu.get_barrier_semaphore()
    for k in range(1, 8):
        pl.semaphore_signal(bar, inc=1, device_id=at_flat(k)[1], device_id_type=MESH)
    pl.semaphore_wait(bar, 7)

    def ocp(b):
        return rdma(o_ref.at[blk(b)], oall.at[blk(b)], osem.at[0, b], osem.at[1, b], ypeer)

    ins[0].wait()
    ocp(0).start()
    ocp(1).start()

    def d2d_cp(u, p, r):
        xq = 1 - x if p == 0 else x
        return rdma(acc.at[1 - c, xq, blk(r), :], dd.at[xq, blk(r), :], d2d.at[u, p, 0, r], d2d.at[u, p, 1, r], cpeer)

    def x_cp(u, r):
        return rdma(xs.at[blk(r)], xr.at[blk(r)], xx.at[u, 0, r], xx.at[u, 1, r], xpeer)

    def agc_cp(u, r, buf):
        return rdma(buf.at[tp, blk(r)], buf.at[tp, blk(r)], agc.at[u, 0, r], agc.at[u, 1, r], cpeer)

    def agx_cp(u, r, buf):
        return rdma(buf.at[tp, blk(r)], buf.at[tp, blk(r)], agx.at[u, 0, r], agx.at[u, 1, r], xpeer)

    def fwd_cp(u, r, buf):
        q = lax.rem(tp + 2, 4)
        return rdma(buf.at[q, blk(r)], buf.at[q, blk(r)], fwd.at[u, 0, r], fwd.at[u, 1, r], cpeer)

    def chip_sum(u, r):
        d2d_cp(u, 0, r).wait_recv()
        xs[blk(r), :] = acc[c, 1 - x, blk(r), :] + dd[1 - x, blk(r), :]
        x_cp(u, r).start()

    def total(u, r):
        d2d_cp(u, 1, r).wait_recv()
        x_cp(u, r).wait_recv()
        return (acc[c, x, blk(r), :] + dd[x, blk(r), :] + xr[blk(r), :]).astype(BF16)

    def gather(u, r, buf):
        agx_cp(u, r, buf).start()
        agc_cp(u, r, buf).start()

    def relay(u, r, buf):
        agx_cp(u, r, buf).wait_recv()
        fwd_cp(u, r, buf).start()

    def arrived(u, r, buf):
        agc_cp(u, r, buf).wait_recv()
        fwd_cp(u, r, buf).wait_recv()

    def drained(u, r, buf):
        d2d_cp(u, 0, r).wait_send()
        d2d_cp(u, 1, r).wait_send()
        x_cp(u, r).wait_send()
        agc_cp(u, r, buf).wait_send()
        agx_cp(u, r, buf).wait_send()
        fwd_cp(u, r, buf).wait_send()

    def zero_acc():
        for a in range(2):
            for b in range(2):
                acc[a, b] = jnp.zeros((128, 1024), F32)

    def acc_cols(n):
        q = n // 2
        return q % 2, q // 2, slice((n % 2) * 512, (n % 2) * 512 + 512)

    def wo_piece(src, n, rs):
        at = opiece(n)
        cols = pl.ds(pl.multiple_of(at * 512, 512), 512)
        v = jnp.dot(src[:, 0:C], dbuf[0, :, cols], preferred_element_type=F32)
        for j in range(1, 8):
            v += jnp.dot(src[:, j * C:(j + 1) * C], dbuf[j, :, cols], preferred_element_type=F32)
        q = at // 2
        for i, r in enumerate(rs):
            acc[lax.rem(q, 2), q // 2, blk(r), (n % 2) * 512:(n % 2) * 512 + 512] = v[i * RB:i * RB + RB]

    def own(ns):
        for n in ns:
            ocopy(n).wait()
            wo_piece(o_ref, n, (0, 2))

    def peers(r, ns):
        for n in ns:
            wo_piece(oall.at[blk(r // 2)], n, (r,))

    own(range(4))
    d2d_cp(0, 0, 0).start()
    d2d_cp(0, 0, 2).start()
    own((4, 5))
    chip_sum(0, 0)
    own((6, 7))
    d2d_cp(0, 1, 0).start()
    d2d_cp(0, 1, 2).start()
    for t in range(2):
        wcopy0(0, t).start()
    for s in range(1, NB):
        for t in range(2):
            wcopy(s, s, t).start()
    ocp(0).wait_recv()
    peers(1, range(4))
    d2d_cp(0, 0, 1).start()
    peers(1, (4, 5))
    chip_sum(0, 1)
    peers(1, (6, 7))
    d2d_cp(0, 1, 1).start()
    ins[1].wait()
    ins[2].wait()
    qcols = pl.ds(pl.multiple_of(tp * 1024, 1024), 1024)

    def h_mid(r):
        att = total(0, r)
        h1 = (hid[rows_of(r), qcols].astype(F32) + att.astype(F32)).astype(BF16)
        hq[tp, blk(r)] = h1
        gather(0, r, hq)
        h32 = h1.astype(F32)
        return jnp.sum(h32 * h32, axis=-1, keepdims=True)

    def st_cp(b, k, own):
        f, dev = at_flat(k)
        if own:
            return rdma(st.at[b, flat], st.at[b, flat], stsem.at[b, 0, f], stsem.at[b, 1, flat], dev)
        return rdma(st.at[b, f], st.at[b, f], stsem.at[b, 0, f], stsem.at[b, 1, f], dev)

    def stats(b, sq):
        st[b, flat] = row_to_lanes(jnp.concatenate(sq + [jnp.zeros((64, 1), F32)], axis=0))
        for k in range(1, 8):
            st_cp(b, k, True).start()

    lane = lax.broadcasted_iota(jnp.int32, (8, 128), 1)

    def x2_rows(b):
        for k in range(1, 8):
            st_cp(b, k, False).wait_recv()
        tot = jnp.zeros((8, 128), F32)
        for f in range(8):
            v = st[b, f]
            swapped = jnp.where(lane < RB, pltpu.roll(v, 128 - RB, 1), pltpu.roll(v, RB, 1))
            tot += jnp.where(dm == f // 4, v, swapped)
        scale = lax.rsqrt(lanes_to_row(tot[0:1, :]) / width_full + EPS)[0:64]
        rows = slice(64 * b, 64 * b + 64)
        arrived(0, 2 * b, hq)
        arrived(0, 2 * b + 1, hq)
        for j in range(32):
            x2[rows, 128 * j:128 * j + 128] = (hq[j // 8, rows, 128 * (j % 8):128 * (j % 8) + 128].astype(F32) * scale * gain[j:j + 1, :].astype(F32)).astype(BF16)

    sq0 = h_mid(0)
    ocp(1).wait_recv()
    peers(3, range(4))
    d2d_cp(0, 0, 3).start()
    peers(3, (4, 5))
    stats(0, [sq0, h_mid(1)])
    chip_sum(0, 2)
    peers(3, (6, 7))
    d2d_cp(0, 1, 3).start()
    dcopy0(0).start()
    for d in range(1, ND):
        dcopy(d, d).start()
    relay(0, 0, hq)
    chip_sum(0, 3)
    relay(0, 1, hq)
    x2_rows(0)

    def g_cp(b, ch, w=C):
        return rdma(gsnd.at[b, ch, :, :, 0:w], grcv.at[b, ch, :, :, 0:w], gs.at[b, ch], gr.at[b, ch], ypeer)

    def m_cp(b, ch, w=C):
        return rdma(mall.at[b, ch, 0:RB, 0:w], mall.at[b, ch, RB:2 * RB, 0:w], ms.at[b, ch], mr.at[b, ch], ypeer)

    def up_gate(ch, slot, blocks, w=C):
        lo, hi = blocks[0] * 64, blocks[-1] * 64 + 64
        for t in range(2):
            v = jnp.dot(x2[lo:hi, :], wbuf[slot, t, :, 0:w], preferred_element_type=F32)
            for i, b in enumerate(blocks):
                gown[b, ch, t, :, 0:w] = v[64 * i:64 * i + RB]
                gsnd[b, ch, t, :, 0:w] = v[64 * i + RB:64 * i + 64]

    def act(b, ch, w=C):
        g_cp(b, ch, w).wait_recv()
        g = gown[b, ch, 0, :, 0:w] + grcv[b, ch, 0, :, 0:w]
        u = gown[b, ch, 1, :, 0:w] + grcv[b, ch, 1, :, 0:w]
        mall[b, ch, 0:RB, 0:w] = (g * jax.nn.sigmoid(g) * u).astype(BF16)
        m_cp(b, ch, w).start()

    def down(b, ch, slot, w=C):
        m_cp(b, ch, w).wait_recv()
        m = mall[b, ch, :, 0:w]
        rows = pl.ds(pl.multiple_of(b * 64, 64), 64)

        for n in range(8):
            a, bb, cols = acc_cols(n)
            acc[a, bb, rows, cols] += jnp.dot(m, dbuf[slot, 0:w, n * 512:n * 512 + 512], preferred_element_type=F32)

    sqb = []

    def second_half(step):
        if step == 0:
            sqb.append(h_mid(2))
        elif step == 2:
            sqb.append(h_mid(3))
            stats(1, sqb)
        elif step == 3:
            relay(0, 2, hq)
            relay(0, 3, hq)
        elif step == LEAD - 1:
            x2_rows(1)
            for r in range(NR):
                drained(0, r, hq)
            zero_acc()

    for e in range(LEAD):
        for t in range(2):
            (wcopy0(0, t) if e == 0 else wcopy(e, e, t)).wait()
        up_gate(e, e % NB, [0], 128 if e == 0 else C)
        g_cp(0, e, 128 if e == 0 else C).start()
        for t in range(2):
            wcopy(e + NB, e + NB, t).start()
        if e >= LAG:
            act(0, e - LAG, 128 if e == LAG else C)
        second_half(e)

    def split(e):
        b = e // N
        return b, jnp.where(b == 0, e, bchunk(e - N))

    @pl.loop(LEAD, 2 * N + DLAG)
    def _(e):
        @pl.when(e < N)
        def _():
            for t in range(2):
                wcopy(e, e, t).wait()
            up_gate(e, lax.rem(e, NB), [0, 1])

        @pl.when(e == N)
        def _():
            for t in range(2):
                wcopy0(N, t).wait()
            up_gate(0, N % NB, [1], 128)

        @pl.when((e > N) & (e < N + LEAD))
        def _():
            for t in range(2):
                wcopy(e, e - N, t).wait()
            up_gate(e - N, lax.rem(e, NB), [1])

        @pl.when((e < 2 * N) & (e != BODD))
        def _():
            b, ch = split(e)
            g_cp(b, ch).start()

        @pl.when(e == BODD)
        def _():
            g_cp(1, 0, 128).start()

        s = e + NB

        @pl.when((s < N + LEAD) & (s != N))
        def _():
            for t in range(2):
                wcopy(s, jnp.where(s < N, s, s - N), t).start()

        @pl.when(s == N)
        def _():
            for t in range(2):
                wcopy0(N, t).start()

        i = e - LAG

        @pl.when((i < 2 * N) & (i != BODD))
        def _():
            b, ch = split(i)
            act(b, ch)

        @pl.when(i == BODD)
        def _():
            act(1, 0, 128)

        d = e - DLAG

        @pl.when(d == 0)
        def _():
            dcopy0(0).wait()
            down(0, 0, 0, 128)

        @pl.when(d == BODD)
        def _():
            dcopy0(BODD).wait()
            down(1, 0, BODD % ND, 128)

        @pl.when((d > 0) & (d != BODD))
        def _():
            b, ch = split(d)
            dcopy(d, ch).wait()
            down(b, ch, lax.rem(d, ND))

        f = d + ND

        @pl.when((f < 2 * N) & (f != BODD))
        def _():
            dcopy(f, split(f)[1]).start()

        @pl.when(f == BODD)
        def _():
            dcopy0(BODD).start()

        def res(r):
            mlp = total(1, r)
            oq[tp, blk(r)] = (hq[tp, blk(r)].astype(F32) + mlp.astype(F32)).astype(BF16)
            gather(1, r, oq)

        @pl.when(d == N)
        def _():
            for r in (0, 1):
                d2d_cp(1, 0, r).start()
                d2d_cp(1, 1, r).start()

        @pl.when(d == N + 1)
        def _():
            chip_sum(1, 0)
            chip_sum(1, 1)

        @pl.when(d == N + 5)
        def _():
            res(0)

        @pl.when(d == N + 7)
        def _():
            res(1)

        @pl.when(d == N + 10)
        def _():
            relay(1, 0, oq)
            relay(1, 1, oq)

    for r in (2, 3):
        d2d_cp(1, 0, r).start()
    for r in (2, 3):
        d2d_cp(1, 1, r).start()
    for r in (2, 3):
        chip_sum(1, r)

    def put(r):
        return pltpu.make_async_copy(outv.at[rows_of(r)], out.at[rows_of(r)], outsem.at[r])

    def emit(r):
        arrived(1, r, oq)
        for q in range(4):
            outv[rows_of(r), 1024 * q:1024 * q + 1024] = oq[q, blk(r), :]
        put(r).start()

    emit(0)
    emit(1)
    for r in (2, 3):
        mlp = total(1, r)
        oq[tp, blk(r)] = (hq[tp, blk(r)].astype(F32) + mlp.astype(F32)).astype(BF16)
        gather(1, r, oq)
    for r in (2, 3):
        relay(1, r, oq)
    for b in range(2):
        for k in range(1, 8):
            st_cp(b, k, True).wait_send()
        ocp(b).wait_send()
        g_cp(b, 0, 128).wait_send()
        m_cp(b, 0, 128).wait_send()

    @pl.loop(1, N)
    def _(ch):
        for b in range(2):
            g_cp(b, ch).wait_send()
            m_cp(b, ch).wait_send()

    emit(2)
    emit(3)
    for r in range(NR):
        drained(1, r, oq)
        put(r).wait()


def mlp_call(o, hidden, gain, wo, wg, wu, wd, width_full):
    dma = pltpu.SemaphoreType.DMA
    return pl.pallas_call(
        functools.partial(mlp_kernel, width_full),
        out_shape=jax.ShapeDtypeStruct((128, 4096), BF16),
        in_specs=[HB] * 7, out_specs=HB,
        scratch_shapes=[
            pltpu.VMEM((64, 2048), BF16), pltpu.VMEM((128, 4096), BF16), pltpu.VMEM((32, 128), BF16), dma((3,)),
            pltpu.VMEM((128, 4096), BF16), dma((NR,)),
            pltpu.VMEM((NB, 2, 4096, C), BF16),
            pltpu.VMEM((ND, C, 4096), BF16),
            pltpu.VMEM((64, 2048), BF16),
            pltpu.VMEM((2, 2, 128, 1024), F32),
            pltpu.VMEM((2, 128, 1024), F32),
            pltpu.VMEM((128, 1024), F32),
            pltpu.VMEM((128, 1024), F32),
            pltpu.VMEM((4, 128, 1024), BF16),
            pltpu.VMEM((4, 128, 1024), BF16),
            pltpu.VMEM((128, 4096), BF16),
            pltpu.VMEM((2, N, 2, RB, C), F32),
            pltpu.VMEM((2, N, 2, RB, C), F32),
            pltpu.VMEM((2, N, 2, RB, C), F32),
            pltpu.VMEM((2, N, 2 * RB, C), BF16),
            pltpu.VMEM((2, 8, 8, 128), F32),
            dma((NB, 2)), dma((ND,)), dma((2, 2)),
            dma((2, 2, 2, NR)), dma((2, 2, NR)), dma((2, 2, NR)), dma((2, 2, NR)), dma((2, 2, NR)),
            dma((2, 2, 8)), dma((2, N)), dma((2, N)), dma((2, N)), dma((2, N)),
        ],
        compiler_params=pltpu.CompilerParams(collective_id=2, has_side_effects=True, vmem_limit_bytes=56 * 2**20),
        name='mlp',
    )(o, hidden, gain, wo, wg, wu, wd)


def copy_kernel(src, dst, buf, isem, osem):
    def part(a, b, sem, i):
        rows = pl.ds(32 * i, 32)
        return pltpu.make_async_copy(a.at[rows], b.at[rows], sem.at[i])

    for i in range(4):
        part(src, buf, isem, i).start()
    for i in range(4):
        part(src, buf, isem, i).wait()
        part(buf, dst, osem, i).start()
    for i in range(4):
        part(buf, dst, osem, i).wait()


def copy_call(h):
    return pl.pallas_call(
        copy_kernel,
        out_shape=jax.ShapeDtypeStruct(h.shape, h.dtype),
        in_specs=[HB], out_specs=HB,
        scratch_shapes=[pltpu.VMEM((128, 4096), BF16), pltpu.SemaphoreType.DMA((4,)), pltpu.SemaphoreType.DMA((4,))],
        name='copy_out',
    )(h)


def solution(mesh):
    width_shards = mesh.shape['dm']
    row_spec = P('dp', 'dm')
    cache_spec = P(('dp', 'dm'), None, 'tp', None)
    batch_spec = P(('dp', 'dm'))
    rope_spec = P(('dp', 'dm'), None)
    in_specs = (row_spec, P('dm', 'tp', None), P('dm', 'tp', None), P('dm', 'tp', None), P('tp', None, 'dm'), P('dm', 'tp'), P('dm', 'tp'), P('tp', 'dm'), P('dm'), P('dm'), cache_spec, cache_spec, batch_spec, rope_spec, rope_spec)
    out_specs = (row_spec, cache_spec, cache_spec)

    def local_layer(hidden, w_q, w_k, w_v, w_o, w_gate, w_up, w_down, norm_attn, norm_mlp, k_cache, v_cache, seq_lens, rope_cos, rope_sin):
        width_full = hidden.shape[1] * width_shards
        q_rot, kv_new = qkv_call(hidden, norm_attn.reshape(-1, 128), rope_cos, rope_sin, w_q.reshape(-1, 128), w_k.reshape(-1, 128), w_v.reshape(-1, 128), width_full)
        k_out, v_out, o = attn_call(q_rot, kv_new, seq_lens, k_cache.reshape(64, 256, 128), v_cache.reshape(64, 256, 128))
        h_out = mlp_call(o, hidden, norm_mlp.reshape(-1, 128), w_o.reshape(8, 256, -1), w_gate, w_up, w_down, width_full)
        h_out = copy_call(h_out)
        return h_out, k_out.reshape(k_cache.shape), v_out.reshape(v_cache.shape)

    return jax.shard_map(local_layer, mesh=mesh, in_specs=in_specs, out_specs=out_specs, check_vma=False)
```
